32 devices in a mesh: fsdp: 4 (over y, core), grp: 8 (over z, x).
Axes of the slice: x: 2, y: 2, z: 4, core: 2. Of those that a mesh axis runs over, the one named last changes fastest.
Arguments:
- grad: bfloat16 [8, 512, 2048], P('grp', 'fsdp'), may hold values from -30 to 30
- table: int32 [8, 4], P('grp'), may hold values from 0 to 3, each once within a row
- left_stat: bfloat16 [8, 4, 512, 512], P('grp', 'fsdp'), may hold values from -4 to 4, as said below
- right_stat: bfloat16 [8, 4, 512, 512], P('grp', 'fsdp'), may hold values from -4 to 4, as said below
- left_basis: bfloat16 [8, 4, 512, 512], P('grp', 'fsdp'), may hold values from -4 to 4, as said below
- right_basis: bfloat16 [8, 4, 512, 512], P('grp', 'fsdp'), may hold values from -4 to 4, as said below
- row_moment: float32 [8, 4, 512], P('grp', 'fsdp'), may hold values from 0.05 to 1
- col_moment: float32 [8, 4, 512], P('grp', 'fsdp'), may hold values from 0.05 to 1
Outputs:
- update: bfloat16 [8, 512, 2048], P('grp', 'fsdp')
- row_next: float32 [8, 4, 512], P('grp', 'fsdp')
- col_next: float32 [8, 4, 512], P('grp', 'fsdp')
The draws below stay inside these ranges and needn't reach their ends.
Inputs may be any that keep to these rules, and one draw needn't show every extreme that they name: Each row of table lists every owner 0 to 3 once. `left_stat`: symmetric with a dominant diagonal. `right_stat`: symmetric with a dominant diagonal. `left_basis`: nonsingular. `right_basis`: nonsingular.
All inputs are finite; a program needn't handle non-finite values.
Results may differ from the reference program's by a relative error of at most 0.01.
Values may be sent and summed in bfloat16 or wider, within the bound.
A program may use at most 64 MiB of HBM per device.

```python
import math
import jax
import jax.numpy as jnp
from jax import lax

B = 512
NF = 4
GROUPS = 8


def symmetric_draw(key):
    noise = jax.random.normal(key, (GROUPS, NF, B, B), jnp.float32)
    sym = (noise + jnp.swapaxes(noise, 2, 3)) / jnp.sqrt(2.0)
    spread = 0.5
    result = 2.0 * jnp.eye(B, dtype=jnp.float32) + spread / jnp.sqrt(1.0 * B) * sym
    return jnp.clip(result, -4.0, 4.0).astype(jnp.bfloat16)


def basis_draw(key):
    noise = jax.random.normal(key, (GROUPS, NF, B, B), jnp.float32)
    spread = 0.5
    result = jnp.eye(B, dtype=jnp.float32) + spread / jnp.sqrt(1.0 * B) * noise
    return jnp.clip(result, -4.0, 4.0).astype(jnp.bfloat16)


def draw_grad(key, part):
    inner_key = jax.random.fold_in(key, 21)
    base = jnp.clip(jax.random.normal(inner_key, (GROUPS, B, NF * B), jnp.float32), -6.0, 6.0)
    lowest = 0.4
    highest = 2.0
    group_scale = jnp.exp(jnp.linspace(jnp.log(lowest), jnp.log(highest), GROUPS, dtype=jnp.float32))
    row_scale = jnp.exp(jnp.linspace(jnp.log(0.6), jnp.log(1.5), B, dtype=jnp.float32))
    result = base * group_scale[:, None, None] * row_scale[None, :, None]
    return result.astype(jnp.bfloat16)


def draw_left_stat(key, part):
    return symmetric_draw(jax.random.fold_in(key, 11))


def draw_right_stat(key, part):
    return symmetric_draw(jax.random.fold_in(key, 12))


def draw_left_basis(key, part):
    return basis_draw(jax.random.fold_in(key, 13))


def draw_right_basis(key, part):
    return basis_draw(jax.random.fold_in(key, 14))


def shard_levels(stream_key, dims, split, smallest, high):
    level = 1.0
    for position, blocks in split:
        heights = jax.random.uniform(jax.random.fold_in(jax.random.fold_in(stream_key, 6), position), (blocks,), jnp.float32, smallest / len(split), high / len(split))
        level = level * jnp.repeat(jnp.exp(heights), dims[position] // blocks).reshape((-1,) + (1,) * (len(dims) - 1 - position))
    return level


def setup_inputs(seed: int = 0) -> dict:
    splits = jax.random.split(jax.random.key(seed), 9)
    grad = draw_grad(jax.random.fold_in(splits[8], 71), 0)
    table = jax.vmap(lambda own: jax.random.permutation(own, NF))(jax.random.split(splits[1], GROUPS)).reshape((GROUPS, NF)).astype(jnp.int32)
    left_stat = draw_left_stat(jax.random.fold_in(splits[8], 71), 0)
    right_stat = draw_right_stat(jax.random.fold_in(splits[8], 71), 0)
    left_basis = draw_left_basis(jax.random.fold_in(splits[8], 71), 0)
    right_basis = draw_right_basis(jax.random.fold_in(splits[8], 71), 0)
    row_moment = jnp.clip(jnp.exp(math.log(1.0) - 2.9957323 * jax.random.uniform(splits[6], (GROUPS, NF, B), jnp.float32) ** shard_levels(splits[6], (GROUPS, NF, B), ((0, 8), (1, 4)), -0.2, 0.2)), 0.05, 1.0)
    col_moment = jnp.clip(jnp.exp(math.log(1.0) - 2.9957323 * jax.random.uniform(splits[7], (GROUPS, NF, B), jnp.float32) ** shard_levels(splits[7], (GROUPS, NF, B), ((0, 8), (1, 4)), -0.2, 0.2)), 0.05, 1.0)
    return {"grad": grad, "table": table, "left_stat": left_stat, "right_stat": right_stat, "left_basis": left_basis, "right_basis": right_basis, "row_moment": row_moment, "col_moment": col_moment}


DECAY_STAT = 0.95
DECAY_MOMENT = 0.95
CLIP_RMS = 0.5
EPSILON = 1e-08

def refresh(stat, gram, basis, clip):
    new_stat = DECAY_STAT * stat.astype(jnp.float32) + (1.0 - DECAY_STAT) * clip * clip * gram
    product = jnp.dot(new_stat, basis.astype(jnp.float32), precision=lax.Precision.HIGHEST)
    inner = jnp.dot(product.T, product, precision=lax.Precision.HIGHEST)
    factor = jnp.linalg.cholesky(inner)
    ortho = jax.scipy.linalg.solve_triangular(factor, product.T, lower=True).T
    return ortho.astype(jnp.bfloat16)

def soap_block(block, clip, left_stat, right_stat, left_basis, right_basis, row_moment, col_moment):
    left_gram = jnp.dot(block.astype(jnp.float32), block.T.astype(jnp.float32), preferred_element_type=jnp.float32)
    right_gram = jnp.dot(block.T.astype(jnp.float32), block.astype(jnp.float32), preferred_element_type=jnp.float32)
    left_new = refresh(left_stat, left_gram, left_basis, clip)
    right_new = refresh(right_stat, right_gram, right_basis, clip)
    half = jnp.dot(left_new.T.astype(jnp.float32), block.astype(jnp.float32), preferred_element_type=jnp.float32).astype(jnp.bfloat16)
    rotated = clip * jnp.dot(half.astype(jnp.float32), right_new.astype(jnp.float32), preferred_element_type=jnp.float32)
    square = rotated * rotated
    row_next = DECAY_MOMENT * row_moment + (1.0 - DECAY_MOMENT) * lax.optimization_barrier(jnp.mean(square, axis=1))
    col_next = DECAY_MOMENT * col_moment + (1.0 - DECAY_MOMENT) * lax.optimization_barrier(jnp.mean(square, axis=0))
    second = row_next[:, None] * col_next[None, :] / jnp.mean(row_next)
    normed = (rotated / (jnp.sqrt(second) + EPSILON)).astype(jnp.bfloat16)
    back = jnp.dot(left_new.astype(jnp.float32), normed.astype(jnp.float32), preferred_element_type=jnp.float32).astype(jnp.bfloat16)
    update = jnp.dot(back.astype(jnp.float32), right_new.T.astype(jnp.float32), preferred_element_type=jnp.float32).astype(jnp.bfloat16)
    return (update, row_next, col_next)

def reference(grad, table, left_stat, right_stat, left_basis, right_basis, row_moment, col_moment):
    total = jnp.sum(jnp.square(grad.astype(jnp.float32)))
    count = GROUPS * NF * B * B
    clip = CLIP_RMS / jnp.sqrt(total / count + 1e-06)
    inverse = jnp.argsort(table, axis=1).astype(jnp.int32).reshape(GROUPS * NF)
    groups_of = (jnp.arange(GROUPS * NF, dtype=jnp.int32) // NF).astype(jnp.int32)

    def one_owner(items):
        group, column, lstat, rstat, lbasis, rbasis, rmom, cmom = items
        start = (column * B).astype(jnp.int32)
        block = lax.dynamic_slice(grad, (group, jnp.int32(0), start), (1, B, B))[0]
        return soap_block(block, clip, lstat, rstat, lbasis, rbasis, rmom, cmom)
    blocks, row_next, col_next = lax.map(one_owner, (groups_of, inverse, left_stat.reshape(GROUPS * NF, B, B), right_stat.reshape(GROUPS * NF, B, B), left_basis.reshape(GROUPS * NF, B, B), right_basis.reshape(GROUPS * NF, B, B), row_moment.reshape(GROUPS * NF, B), col_moment.reshape(GROUPS * NF, B)))
    blocks = blocks.reshape(GROUPS, NF, B, B)
    by_column = jnp.take_along_axis(blocks, table[:, :, None, None].astype(jnp.int32), axis=1)
    update = by_column.transpose(0, 2, 1, 3).reshape(GROUPS, B, NF * B)
    return (update, row_next.reshape(GROUPS, NF, B), col_next.reshape(GROUPS, NF, B))
```

```python
import functools
import jax
import jax.numpy as jnp
from jax import lax
from jax.experimental import pallas as pl
from jax.experimental.pallas import tpu as pltpu
from jax.sharding import PartitionSpec as P

DECAY_STAT = 0.95
DECAY_MOMENT = 0.95
CLIP_RMS = 0.5
EPSILON = 1e-08
OUTER = 128
INNER = 32
PANEL = 16

NN = (((1,), (0,)), ((), ()))
NT = (((1,), (1,)), ((), ()))
TN = (((0,), (0,)), ((), ()))
MESH = pl.DeviceIdType.MESH


def mm(a, b, dims=NN):
    return lax.dot_general(a, b, dims, preferred_element_type=jnp.float32)


def mm_high(a, b, dims=NN):
    return lax.dot_general(a, b, dims, preferred_element_type=jnp.float32, precision=lax.Precision.HIGHEST)


def split(a):
    high = a.astype(jnp.bfloat16)
    return high, (a - high.astype(jnp.float32)).astype(jnp.bfloat16)


def mm_split(a, b, dims=NN):
    return mm(a[0], b[0], dims) + (mm(a[0], b[1], dims) + mm(a[1], b[0], dims))


def eliminate(pack):
    lane = lax.broadcasted_iota(jnp.int32, pack.shape, 1)
    row = lax.broadcasted_iota(jnp.int32, pack.shape, 0)
    low = lane < 2 * INNER
    scale = jnp.ones_like(pack)
    done = []
    rest = pack
    for start in range(0, INNER, PANEL):
        shape = rest.shape
        below = lax.broadcasted_iota(jnp.int32, shape, 0)
        half = low[: shape[0]]
        columns = [
            jnp.where(
                half,
                jnp.broadcast_to(rest[:, j : j + 1], shape),
                jnp.broadcast_to(rest[:, 2 * INNER + j : 2 * INNER + j + 1], shape),
            )
            for j in range(start, start + PANEL)
        ]
        head_scale = jnp.ones((PANEL, shape[1]), jnp.float32)
        for p in range(PANEL):
            pivot = columns[p][p : p + 1, :]
            root = lax.rsqrt(pivot)
            inverse = root * root
            factor = jnp.where(below > p, columns[p], 0.0) * inverse
            for q in range(p + 1, PANEL):
                columns[q] = columns[q] - factor * columns[q][p : p + 1, :]
            rest = rest - factor * rest[p : p + 1, :]
            head_scale = jnp.where(below[:PANEL] == p, root, head_scale)
        done.append(rest[:PANEL] * head_scale)
        rest = rest[PANEL:]
    return jnp.concatenate(done, axis=0)


def inverse_factors(grams, work):
    row = lax.broadcasted_iota(jnp.int32, (OUTER, OUTER), 0)
    col = lax.broadcasted_iota(jnp.int32, (OUTER, OUTER), 1)
    eye = jnp.where(row == col, 1.0, 0.0)
    for c in range(2):
        work[c, :, :OUTER] = grams[c]
        work[c, :, OUTER:] = eye
    small_row = lax.broadcasted_iota(jnp.int32, (INNER, OUTER), 0)
    lane = lax.broadcasted_iota(jnp.int32, (INNER, OUTER), 1)
    small_eye = jnp.where((lane == small_row + INNER) | (lane == small_row + 3 * INNER), 1.0, 0.0)
    for b in range(OUTER // INNER):
        rows = pl.ds(b * INNER, INNER)
        left = work[0, rows, :OUTER]
        right = work[1, rows, :OUTER]
        if b:
            left = pltpu.roll(left, OUTER - b * INNER, 1)
        shift = (2 * INNER - b * INNER) % OUTER
        if shift:
            right = pltpu.roll(right, shift, 1)
        pack = jnp.where(lane < INNER, left, small_eye)
        pack = jnp.where((lane >= 2 * INNER) & (lane < 3 * INNER), right, pack)
        pack = eliminate(pack)
        for c in range(2):
            factor = pltpu.roll(pack, OUTER - INNER if c == 0 else INNER, 1)[:, :INNER]
            solved = mm_split(split(factor), split(work[c, rows, :]))
            work[c, rows, :] = solved
            if (b + 1) * INNER < OUTER:
                tail = pl.ds((b + 1) * INNER, OUTER - (b + 1) * INNER)
                high, low = split(solved)
                cut = slice((b + 1) * INNER, OUTER)
                work[c, tail, :] = work[c, tail, :] - mm_split((high[:, cut], low[:, cut]), (high, low), TN)
    return [work[c, :, OUTER:] for c in range(2)]


def partners(owners):
    return [(chip, core) for chip in range(owners // 2 - 1, -1, -1) for core in (1, 0) if chip or core]


def soap_kernel(
    groups, table_hbm, grad_hbm, ls_hbm, rs_hbm, lb_hbm, rb_hbm, rm_hbm, cm_hbm, out_ref, rn_ref, cn_ref,
    table_ref, grad_ref, rm_ref, cm_ref,
    stat_ref, basis_ref, send_ref, block_ref, back_ref, ret_ref, sums_ref, totals_ref, part_ref,
    x_ref, q_ref, work,
    load_sem, stripe_send, stripe_recv, sum_send, sum_recv, total_send, total_recv, slab_send, slab_recv,
):
    owners, my_rows, order = send_ref.shape
    me = lax.axis_index("fsdp")
    group = lax.axis_index("grp")
    offsets = partners(owners)

    def peer(offset):
        return lax.rem(me // 2 + offset[0], owners // 2) * 2 + lax.rem(me + offset[1], 2)

    def group_peer(step):
        return lax.rem(group + step, groups)

    loads = []

    def load(source, target):
        loads.append(pltpu.make_async_copy(source, target, load_sem.at[len(loads)]))
        loads[-1].start()
        return loads[-1]

    gradient = [load(table_hbm, table_ref)]
    for j in range(owners):
        gradient.append(load(grad_hbm.at[:, pl.ds(j * order, order)], grad_ref.at[j]))
    left = [load(lb_hbm, basis_ref.at[0]), load(ls_hbm, stat_ref.at[0])]
    right = [load(rb_hbm, basis_ref.at[1]), load(rs_hbm, stat_ref.at[1])]
    moments = [load(rm_hbm, rm_ref), load(cm_hbm, cm_ref)]
    barrier = pltpu.get_barrier_semaphore()
    for offset in offsets:
        pl.semaphore_signal(barrier, inc=1, device_id={"fsdp": peer(offset)}, device_id_type=MESH)
    for step in range(1, groups):
        pl.semaphore_signal(barrier, inc=1, device_id={"grp": group_peer(step)}, device_id_type=MESH)
    for copy in gradient:
        copy.wait()

    def stripe(owner):
        column = jnp.int32(0)
        for j in range(1, owners):
            column = jnp.where(table_ref[0, j] == owner, j, column)
        return grad_ref[column]

    for offset in offsets:
        owner = peer(offset)
        send_ref[owner] = stripe(owner)
    my_slab = pl.ds(pl.multiple_of(me * my_rows, my_rows), my_rows)
    block_ref[my_slab, :] = stripe(me)
    local = jnp.zeros((1, order), jnp.float32)
    for j in range(owners):
        piece = grad_ref[j].astype(jnp.float32)
        local = local + jnp.sum(piece * piece, axis=0, keepdims=True)
    local = jnp.broadcast_to(jnp.sum(local, axis=1, keepdims=True), sums_ref.shape[1:])
    part_ref[0] = local
    sums_ref[me] = local
    pl.semaphore_wait(barrier, owners - 1 + groups - 1)

    sum_copies, stripe_copies, total_copies, slab_copies = [], [], [], []
    for i, offset in enumerate(offsets):
        sum_copies.append(
            pltpu.make_async_remote_copy(
                src_ref=part_ref.at[0], dst_ref=sums_ref.at[me], send_sem=sum_send.at[i], recv_sem=sum_recv.at[i],
                device_id={"fsdp": peer(offset)}, device_id_type=MESH,
            )
        )
        sum_copies[-1].start()
    for i, offset in enumerate(offsets):
        stripe_copies.append(
            pltpu.make_async_remote_copy(
                src_ref=send_ref.at[peer(offset)], dst_ref=block_ref.at[my_slab, :],
                send_sem=stripe_send.at[i], recv_sem=stripe_recv.at[i],
                device_id={"fsdp": peer(offset)}, device_id_type=MESH,
            )
        )
        stripe_copies[-1].start()
    for copy in left:
        copy.wait()
    x_ref[0] = mm(basis_ref[0], stat_ref[0], TN)
    for copy in sum_copies:
        copy.wait_recv()
    matrix_sum = sums_ref[0]
    for i in range(1, owners):
        matrix_sum = matrix_sum + sums_ref[i]
    part_ref[1] = matrix_sum
    totals_ref[group] = matrix_sum
    for copy in right:
        copy.wait()
    for copy in moments:
        copy.wait()
    for step in range(1, groups):
        total_copies.append(
            pltpu.make_async_remote_copy(
                src_ref=part_ref.at[1], dst_ref=totals_ref.at[group],
                send_sem=total_send.at[step - 1], recv_sem=total_recv.at[step - 1],
                device_id={"grp": group_peer(step)}, device_id_type=MESH,
            )
        )
        total_copies[-1].start()
    x_ref[1] = mm(basis_ref[1], stat_ref[1], TN)
    for copy in stripe_copies:
        copy.wait_recv()
    g = block_ref[...]
    grams = [split(mm(g, g, dims)) for dims in (NT, TN)]
    for copy in total_copies:
        copy.wait_recv()
    total = totals_ref[0]
    for i in range(1, groups):
        total = total + totals_ref[i]
    count = float(groups * owners * order * order)
    clip = (CLIP_RMS / jnp.sqrt(total / count + 1e-06))[:1, :1]
    weight = (1.0 - DECAY_STAT) * clip * clip
    for c in range(2):
        high, low = grams[c]
        product = mm(basis_ref[c], high, TN) + mm(basis_ref[c], low, TN)
        x_ref[c] = DECAY_STAT * x_ref[c] + weight * product
    for k in range(order // OUTER):
        rows = pl.ds(k * OUTER, OUTER)
        grams = []
        for c in range(2):
            grams.append(mm_high(x_ref[c, rows, :], x_ref[c, rows, :], NT))
        factors = inverse_factors(grams, work)
        for c in range(2):
            block = mm_split(split(factors[c]), split(x_ref[c, rows, :]))
            q_ref[c, rows, :] = block.astype(jnp.bfloat16)
            if (k + 1) * OUTER < order:
                parts = split(block)
                near, far = (k + 1) * OUTER, (k + 2) * OUTER
                for tail in (pl.ds(near, OUTER), pl.ds(far, order - far)):
                    if tail.size:
                        along = mm_split(split(x_ref[c, tail, :]), parts, NT)
                        x_ref[c, tail, :] = x_ref[c, tail, :] - mm_split(split(along), parts)
    half = mm(q_ref[0], g).astype(jnp.bfloat16)
    rotated = clip * mm(half, q_ref[1], NT)
    square = rotated * rotated
    lanes = 128
    mean_row = jnp.broadcast_to(jnp.mean(square, axis=1, keepdims=True), (order, lanes))
    mean_col = jnp.mean(square, axis=0, keepdims=True)
    row_next = DECAY_MOMENT * jnp.broadcast_to(rm_ref[...], (lanes, order)) + (1.0 - DECAY_MOMENT) * mean_row.T
    col_next = DECAY_MOMENT * cm_ref[...] + (1.0 - DECAY_MOMENT) * mean_col
    rn_ref[...] = row_next[:1]
    cn_ref[...] = col_next
    second = row_next.T[:, :1] * col_next / jnp.mean(row_next[:1])
    normed = (rotated / (jnp.sqrt(second) + EPSILON)).astype(jnp.bfloat16)
    back_ref[...] = mm(q_ref[0], normed, TN).astype(jnp.bfloat16)
    for copy in stripe_copies:
        copy.wait_send()

    def slab(owner):
        rows = pl.ds(pl.multiple_of(owner * my_rows, my_rows), my_rows)
        return mm(back_ref[rows, :], q_ref[1]).astype(jnp.bfloat16)

    for i, offset in enumerate(offsets):
        send_ref[peer(offset)] = slab(peer(offset))
        slab_copies.append(
            pltpu.make_async_remote_copy(
                src_ref=send_ref.at[peer(offset)], dst_ref=ret_ref.at[me],
                send_sem=slab_send.at[i], recv_sem=slab_recv.at[i],
                device_id={"fsdp": peer(offset)}, device_id_type=MESH,
            )
        )
        if i:
            slab_copies[i - 1].start()
    ret_ref[me] = slab(me)
    slab_copies[-1].start()
    for copy in slab_copies:
        copy.wait_recv()
    for j in range(owners):
        out_ref[:, j * order : (j + 1) * order] = ret_ref[table_ref[0, j]]
    for copy in sum_copies + total_copies + slab_copies:
        copy.wait_send()


def store_kernel(update_ref, rn_ref, cn_ref, update_hbm, rn_hbm, cn_hbm, sem):
    copies = [
        pltpu.make_async_copy(source, target, sem.at[i])
        for i, (source, target) in enumerate(((update_ref, update_hbm), (rn_ref, rn_hbm), (cn_ref, cn_hbm)))
    ]
    for copy in copies:
        copy.start()
    for copy in copies:
        copy.wait()


def shards(grad, table, left_stat, right_stat, left_basis, right_basis, row_moment, col_moment):
    order = left_stat.shape[-1]
    owners = lax.axis_size("fsdp")
    groups = lax.axis_size("grp")
    my_rows = grad.shape[1]
    vmem = pl.BlockSpec(memory_space=pltpu.VMEM)
    hbm = pl.BlockSpec(memory_space=pltpu.HBM)
    dma = pltpu.SemaphoreType.DMA
    update, row_next, col_next = pl.pallas_call(
        functools.partial(soap_kernel, groups),
        out_shape=(
            jax.ShapeDtypeStruct((my_rows, owners * order), jnp.bfloat16),
            jax.ShapeDtypeStruct((1, order), jnp.float32),
            jax.ShapeDtypeStruct((1, order), jnp.float32),
        ),
        in_specs=[hbm] * 8,
        out_specs=(vmem, vmem, vmem),
        scratch_shapes=[
            pltpu.SMEM((1, owners), jnp.int32),
            pltpu.VMEM((owners, my_rows, order), jnp.bfloat16),
            pltpu.VMEM((1, order), jnp.float32),
            pltpu.VMEM((1, order), jnp.float32),
            pltpu.VMEM((2, order, order), jnp.bfloat16),
            pltpu.VMEM((2, order, order), jnp.bfloat16),
            pltpu.VMEM((owners, my_rows, order), jnp.bfloat16),
            pltpu.VMEM((order, order), jnp.bfloat16),
            pltpu.VMEM((order, order), jnp.bfloat16),
            pltpu.VMEM((owners, my_rows, order), jnp.bfloat16),
            pltpu.VMEM((owners, 8, 128), jnp.float32),
            pltpu.VMEM((groups, 8, 128), jnp.float32),
            pltpu.VMEM((2, 8, 128), jnp.float32),
            pltpu.VMEM((2, order, order), jnp.float32),
            pltpu.VMEM((2, order, order), jnp.bfloat16),
            pltpu.VMEM((2, OUTER, 2 * OUTER), jnp.float32),
            dma((owners + 7,)),
            dma((owners - 1,)),
            dma((owners - 1,)),
            dma((owners - 1,)),
            dma((owners - 1,)),
            dma((groups - 1,)),
            dma((groups - 1,)),
            dma((owners - 1,)),
            dma((owners - 1,)),
        ],
        compiler_params=pltpu.CompilerParams(
            collective_id=0, has_side_effects=True, vmem_limit_bytes=48 * 1024 * 1024
        ),
        name="soap",
    )(
        *[pltpu.with_memory_space_constraint(v, pltpu.HBM) for v in (table, grad[0], left_stat[0, 0], right_stat[0, 0], left_basis[0, 0], right_basis[0, 0],
        row_moment[0], col_moment[0])]
    )
    update, row_next, col_next = pl.pallas_call(
        store_kernel,
        out_shape=tuple(jax.ShapeDtypeStruct(a.shape, a.dtype) for a in (update, row_next, col_next)),
        in_specs=[vmem] * 3,
        out_specs=[hbm] * 3,
        scratch_shapes=[dma((3,))],
        compiler_params=pltpu.CompilerParams(vmem_limit_bytes=4 * 1024 * 1024),
        name="store",
    )(update, row_next, col_next)
    return (update[None], row_next[None], col_next[None])


def solution(mesh):
    in_specs = (
        P("grp", "fsdp", None),
        P("grp", None),
        P("grp", "fsdp", None, None),
        P("grp", "fsdp", None, None),
        P("grp", "fsdp", None, None),
        P("grp", "fsdp", None, None),
        P("grp", "fsdp", None),
        P("grp", "fsdp", None),
    )
    out_specs = (P("grp", "fsdp", None), P("grp", "fsdp", None), P("grp", "fsdp", None))
    return jax.shard_map(shards, mesh=mesh, in_specs=in_specs, out_specs=out_specs, check_vma=False)
```

```python
import functools
import jax
import jax.numpy as jnp
from jax import lax
from jax.experimental import pallas as pl
from jax.experimental.pallas import tpu as pltpu
from jax.sharding import PartitionSpec as P

DECAY_STAT = 0.95
DECAY_MOMENT = 0.95
CLIP_RMS = 0.5
EPSILON = 1e-08
BLOCK = 64
PANEL = 16
SUB = 8

NN = (((1,), (0,)), ((), ()))
NT = (((1,), (1,)), ((), ()))
TN = (((0,), (0,)), ((), ()))
MESH = pl.DeviceIdType.MESH


def mm(a, b, dims=NN):
    return lax.dot_general(a, b, dims, preferred_element_type=jnp.float32)


def split(a):
    high = a.astype(jnp.bfloat16)
    return high, (a - high.astype(jnp.float32)).astype(jnp.bfloat16)


def mm_split(a, b, dims=NN):
    return mm(a[0], b[0], dims) + (mm(a[0], b[1], dims) + mm(a[1], b[0], dims))


def spread(rows, column, sides):
    low, high = (jnp.broadcast_to(rows[:, j : j + 1], rows.shape) for j in (column, BLOCK + column))
    return jnp.where(sides[: rows.shape[0]], low, high)


def invert(pack, pump):
    shape = pack.shape
    lane = lax.broadcasted_iota(jnp.int32, shape, 1)
    row = lax.broadcasted_iota(jnp.int32, shape, 0)
    sides = lane < BLOCK
    local = jnp.where(sides, lane, lane - BLOCK)
    top = row[:SUB]
    done = []
    rest = pack
    for start in range(0, BLOCK, PANEL):
        columns = [spread(rest[q // SUB * SUB :], start + q, sides) for q in range(PANEL)]
        here = local[: rest.shape[0]] - start
        unit = jnp.where(here == row[: rest.shape[0]], 1.0, 0.0)
        rest = jnp.where((here >= 0) & (here < PANEL), unit, rest)
        for p in range(PANEL):
            s = p % SUB
            column = columns[p]
            pivot = column[s : s + 1]
            inverse = 1.0 / pivot
            root = lax.rsqrt(pivot)
            scale = jnp.where(top == s, root, 1.0 if s == 0 else scale)
            factor = jnp.where(top > s, column[:SUB], 0.0)
            if column.shape[0] > SUB:
                factor = jnp.concatenate([factor, column[SUB:]], axis=0)
            factor = factor * inverse
            for q in range(p + 1, PANEL):
                m = q - p + s
                part = factor if q // SUB == p // SUB else factor[SUB:]
                columns[q] = columns[q] - part * column[m : m + 1]
            rest = rest - factor * rest[s : s + 1]
            if s == SUB - 1:
                done.append(rest[:SUB] * scale)
                rest = rest[SUB:]
            pump()
    return jnp.where(local <= row, jnp.concatenate(done, axis=0), 0.0)


def twice(a):
    return jnp.concatenate([a, a], axis=1)


def swap(pieces):
    return [pieces[i ^ 1] for i in range(len(pieces))]


def orthonormalize(strip, x_ref, s_ref, xh_ref, xl_ref, o_ref, m_ref, q_ref, half_ref, g_ref):
    order = x_ref.shape[-1]
    blocks = order // BLOCK
    group = 2 * BLOCK
    lane = lax.broadcasted_iota(jnp.int32, (BLOCK, group), 1)
    first = lane < BLOCK
    queue = []

    def pump(n=1):
        for _ in range(min(n, len(queue))):
            queue.pop(0)()

    def flush():
        pump(len(queue))

    def gram_strip(c, t):
        rows = pl.ds(t * group, group)
        high, low = split(x_ref[c, rows, :])
        xh_ref[c, rows, :] = high
        xl_ref[c, rows, :] = low
        width = (t + 1) * group
        others = []
        for ref in (xh_ref, xl_ref):
            pieces = [ref[c, i * BLOCK : (i + 1) * BLOCK, :] for i in range(width // BLOCK)]
            others.append(jnp.concatenate(swap(pieces) if c else pieces, axis=0))
        s_ref[c, rows, :width] = mm_split((high, low), others, NT)

    def lanes_of(b):
        return slice(b // 2 * group, b // 2 * group + group)

    def packed(b, rows):
        pair = [s_ref[c, rows, lanes_of(b)] for c in range(2)]
        keep = lax.broadcasted_iota(jnp.int32, pair[0].shape, 1) < BLOCK
        return jnp.where(keep, pair[b % 2], pair[1 - b % 2])

    for c in range(2):
        strip(c, 0)
        gram_strip(c, 0)
    for t in range(1, order // group):
        for c in range(2):
            queue.append(functools.partial(strip, c, t))
            queue.append(functools.partial(gram_strip, c, t))
    pack = packed(0, pl.ds(0, BLOCK))
    for b in range(blocks):
        inverse = invert(pack, functools.partial(pump, 1))
        flush()
        own = (first, ~first) if b % 2 == 0 else (~first, first)
        sides = [jnp.where(own[c], inverse, 0.0) for c in range(2)]
        weights = split(jnp.concatenate([sides[0], sides[0], sides[1], sides[1]], axis=0))

        def panel(b, weights, start, stop):
            rows = pl.ds(start, stop - start)
            high, low = split(packed(b, rows))
            o = mm(jnp.concatenate([high, low], axis=1), twice(weights[0]), NT) + mm(high, weights[1], NT)
            high, low = split(o)
            keep = lax.broadcasted_iota(jnp.int32, (stop - start, group), 1) < BLOCK
            for c in range(2):
                cut = slice(c * group, (c + 1) * group)
                o_ref[c, rows, :] = jnp.concatenate([high[:, cut], low[:, cut]], axis=1)
                mixed = jnp.where(keep, high[:, cut].astype(jnp.float32), low[:, cut].astype(jnp.float32)).astype(jnp.bfloat16)
                for i in range(start // BLOCK, stop // BLOCK):
                    place = (i ^ c) * BLOCK
                    m_ref[c, place : place + BLOCK, :] = mixed[i * BLOCK - start : (i + 1) * BLOCK - start]

        def trail(b, c, start, stop):
            rows = pl.ds(start, stop - start)
            near = (b + 1) // 2 * group
            far = -(-stop // group) * group
            cut = slice(near, far)
            s_ref[c, rows, cut] = s_ref[c, rows, cut] - mm(o_ref[c, rows, :], twice(m_ref[c, near:far, :]), NT)

        def finish(b, c, doubled):
            rows = pl.ds(b * BLOCK, BLOCK)
            high, low = split(x_ref[c, rows, :])
            left = jnp.concatenate(split(doubled), axis=1)
            q = mm(left, jnp.concatenate([high, low, high, low], axis=0))
            high, low = split(q)
            q_ref[c, rows, :] = high
            xl_ref[c, rows, :] = low
            if c == 0:
                half_ref[rows, :] = mm(high, g_ref[...]).astype(jnp.bfloat16)

        def deflate(b, c, start, stop):
            rows = pl.ds(start, stop - start)
            done = pl.ds(b * BLOCK, BLOCK)
            high, low = q_ref[c, done, :], xl_ref[c, done, :]
            x_ref[c, rows, :] = x_ref[c, rows, :] - mm(o_ref[c, rows, :], jnp.concatenate([high, low, high, low], axis=0))

        near = (b + 1) * BLOCK
        if near < order:
            if b % 2 == 0:
                for c in range(2):
                    place = (b ^ c) * BLOCK
                    m_ref[c, place : place + BLOCK, :] = jnp.zeros((BLOCK, group), jnp.bfloat16)
            else:
                for c in range(2):
                    place = ((b + 2) ^ c) * BLOCK
                    m_ref[c, place : place + BLOCK, :] = jnp.zeros((BLOCK, group), jnp.bfloat16)
            panel(b, weights, near, near + BLOCK)
            for c in range(2):
                trail(b, c, near, near + BLOCK)
            pack = packed(b + 1, pl.ds(near, BLOCK))
        rolled = pltpu.roll(inverse, BLOCK, 1)
        doubled = [jnp.where(own[c], inverse, rolled) for c in range(2)]
        if near < order:
            chunks = []
            start = near + BLOCK
            while start < order:
                stop = min(order, start // group * group + group)
                chunks.append((start, stop))
                start = stop
            for start, stop in chunks:
                queue.append(functools.partial(panel, b, weights, start, stop))
            for start, stop in chunks:
                for c in range(2):
                    queue.append(functools.partial(trail, b, c, start, stop))
        for c in range(2):
            queue.append(functools.partial(finish, b, c, doubled[c]))
        for start, stop in ([(near, near + BLOCK)] + chunks) if near < order else []:
            for c in range(2):
                queue.append(functools.partial(deflate, b, c, start, stop))
    flush()


def partners(owners):
    return [(chip, core) for chip in range(owners // 2 - 1, -1, -1) for core in (1, 0) if chip or core]


def soap_kernel(
    groups, table_hbm, grad_hbm, ls_hbm, rs_hbm, lb_hbm, rb_hbm, rm_hbm, cm_hbm, out_ref, rn_ref, cn_ref,
    table_ref, grad_ref, rm_ref, cm_ref,
    stat_ref, basis_ref, send_ref, block_ref, ret_ref, sums_ref, totals_ref, part_ref,
    x_ref, q_ref, turned_ref, s_ref, xh_ref, xl_ref, o_ref, m_ref, half_ref,
    load_sem, stripe_send, stripe_recv, sum_send, sum_recv, total_send, total_recv, slab_send, slab_recv,
):
    owners, my_rows, order = send_ref.shape
    me = lax.axis_index("fsdp")
    group = lax.axis_index("grp")
    offsets = partners(owners)

    def peer(offset):
        return lax.rem(me // 2 + offset[0], owners // 2) * 2 + lax.rem(me + offset[1], 2)

    def group_peer(step):
        return lax.rem(group + step, groups)

    loads = []

    def load(source, target):
        loads.append(pltpu.make_async_copy(source, target, load_sem.at[len(loads)]))
        loads[-1].start()
        return loads[-1]

    gradient = [load(table_hbm, table_ref)]
    for j in range(owners):
        gradient.append(load(grad_hbm.at[:, pl.ds(j * order, order)], grad_ref.at[j]))
    left = [load(lb_hbm, basis_ref.at[0]), load(ls_hbm, stat_ref.at[0])]
    right = [load(rb_hbm, basis_ref.at[1]), load(rs_hbm, stat_ref.at[1])]
    moments = [load(rm_hbm, rm_ref), load(cm_hbm, cm_ref)]
    barrier = pltpu.get_barrier_semaphore()
    for offset in offsets:
        pl.semaphore_signal(barrier, inc=1, device_id={"fsdp": peer(offset)}, device_id_type=MESH)
    for step in range(1, groups):
        pl.semaphore_signal(barrier, inc=1, device_id={"grp": group_peer(step)}, device_id_type=MESH)
    for copy in gradient:
        copy.wait()

    def stripe(owner):
        column = jnp.int32(0)
        for j in range(1, owners):
            column = jnp.where(table_ref[0, j] == owner, j, column)
        return grad_ref[column]

    for offset in offsets:
        owner = peer(offset)
        send_ref[owner] = stripe(owner)
    my_slab = pl.ds(pl.multiple_of(me * my_rows, my_rows), my_rows)
    block_ref[my_slab, :] = stripe(me)
    local = jnp.zeros((1, order), jnp.float32)
    for j in range(owners):
        piece = grad_ref[j].astype(jnp.float32)
        local = local + jnp.sum(piece * piece, axis=0, keepdims=True)
    local = jnp.broadcast_to(jnp.sum(local, axis=1, keepdims=True), sums_ref.shape[1:])
    part_ref[0] = local
    sums_ref[me] = local
    pl.semaphore_wait(barrier, owners - 1 + groups - 1)

    sum_copies, stripe_copies, total_copies, slab_copies = [], [], [], []
    for i, offset in enumerate(offsets):
        sum_copies.append(
            pltpu.make_async_remote_copy(
                src_ref=part_ref.at[0], dst_ref=sums_ref.at[me], send_sem=sum_send.at[i], recv_sem=sum_recv.at[i],
                device_id={"fsdp": peer(offset)}, device_id_type=MESH,
            )
        )
        sum_copies[-1].start()
    for i, offset in enumerate(offsets):
        stripe_copies.append(
            pltpu.make_async_remote_copy(
                src_ref=send_ref.at[peer(offset)], dst_ref=block_ref.at[my_slab, :],
                send_sem=stripe_send.at[i], recv_sem=stripe_recv.at[i],
                device_id={"fsdp": peer(offset)}, device_id_type=MESH,
            )
        )
        stripe_copies[-1].start()
    for copy in left:
        copy.wait()
    turned_ref[0] = basis_ref[0].T
    x_ref[0] = mm(turned_ref[0], stat_ref[0])
    for copy in sum_copies:
        copy.wait_recv()
    matrix_sum = sums_ref[0]
    for i in range(1, owners):
        matrix_sum = matrix_sum + sums_ref[i]
    part_ref[1] = matrix_sum
    totals_ref[group] = matrix_sum
    for copy in right:
        copy.wait()
    for copy in moments:
        copy.wait()
    for step in range(1, groups):
        total_copies.append(
            pltpu.make_async_remote_copy(
                src_ref=part_ref.at[1], dst_ref=totals_ref.at[group],
                send_sem=total_send.at[step - 1], recv_sem=total_recv.at[step - 1],
                device_id={"grp": group_peer(step)}, device_id_type=MESH,
            )
        )
        total_copies[-1].start()
    turned_ref[1] = basis_ref[1].T
    x_ref[1] = mm(turned_ref[1], stat_ref[1])
    for copy in stripe_copies:
        copy.wait_recv()
    g = block_ref[...]
    for c, dims in enumerate((NT, TN)):
        stat_ref[c], basis_ref[c] = split(mm(g, g, dims))
    for copy in total_copies:
        copy.wait_recv()
    total = totals_ref[0]
    for i in range(1, groups):
        total = total + totals_ref[i]
    count = float(groups * owners * order * order)
    clip = (CLIP_RMS / jnp.sqrt(total / count + 1e-06))[:1, :1]
    weight = (1.0 - DECAY_STAT) * clip * clip

    def strip(c, t):
        rows = pl.ds(t * 2 * BLOCK, 2 * BLOCK)
        left = turned_ref[c, rows, :]
        product = mm(left, stat_ref[c]) + mm(left, basis_ref[c])
        x_ref[c, rows, :] = DECAY_STAT * x_ref[c, rows, :] + weight * product

    orthonormalize(strip, x_ref, s_ref, xh_ref, xl_ref, o_ref, m_ref, q_ref, half_ref, block_ref)
    half = half_ref[...]
    rotated = clip * mm(half, q_ref[1], NT)
    square = rotated * rotated
    lanes = 128
    mean_row = jnp.broadcast_to(jnp.mean(square, axis=1, keepdims=True), (order, lanes))
    mean_col = jnp.mean(square, axis=0, keepdims=True)
    row_next = DECAY_MOMENT * jnp.broadcast_to(rm_ref[...], (lanes, order)) + (1.0 - DECAY_MOMENT) * mean_row.T
    col_next = DECAY_MOMENT * cm_ref[...] + (1.0 - DECAY_MOMENT) * mean_col
    rn_ref[...] = row_next[:1]
    cn_ref[...] = col_next
    second = row_next.T[:, :1] * col_next / jnp.mean(row_next[:1])
    normed = (rotated / (jnp.sqrt(second) + EPSILON)).astype(jnp.bfloat16)
    block_ref[...] = mm(q_ref[0], normed, TN).astype(jnp.bfloat16)
    for copy in stripe_copies:
        copy.wait_send()

    def slab(owner):
        rows = pl.ds(pl.multiple_of(owner * my_rows, my_rows), my_rows)
        return mm(block_ref[rows, :], q_ref[1]).astype(jnp.bfloat16)

    for i, offset in enumerate(offsets):
        send_ref[peer(offset)] = slab(peer(offset))
        slab_copies.append(
            pltpu.make_async_remote_copy(
                src_ref=send_ref.at[peer(offset)], dst_ref=ret_ref.at[me],
                send_sem=slab_send.at[i], recv_sem=slab_recv.at[i],
                device_id={"fsdp": peer(offset)}, device_id_type=MESH,
            )
        )
        if i:
            slab_copies[i - 1].start()
    ret_ref[me] = slab(me)
    slab_copies[-1].start()
    for copy in slab_copies:
        copy.wait_recv()
    for j in range(owners):
        out_ref[:, j * order : (j + 1) * order] = ret_ref[table_ref[0, j]]
    for copy in sum_copies + total_copies + slab_copies:
        copy.wait_send()


def store_kernel(update_ref, rn_ref, cn_ref, update_hbm, rn_hbm, cn_hbm, sem):
    copies = [
        pltpu.make_async_copy(source, target, sem.at[i])
        for i, (source, target) in enumerate(((update_ref, update_hbm), (rn_ref, rn_hbm), (cn_ref, cn_hbm)))
    ]
    for copy in copies:
        copy.start()
    for copy in copies:
        copy.wait()


def shards(grad, table, left_stat, right_stat, left_basis, right_basis, row_moment, col_moment):
    order = left_stat.shape[-1]
    owners = lax.axis_size("fsdp")
    groups = lax.axis_size("grp")
    my_rows = grad.shape[1]
    vmem = pl.BlockSpec(memory_space=pltpu.VMEM)
    hbm = pl.BlockSpec(memory_space=pltpu.HBM)
    dma = pltpu.SemaphoreType.DMA
    update, row_next, col_next = pl.pallas_call(
        functools.partial(soap_kernel, groups),
        out_shape=(
            jax.ShapeDtypeStruct((my_rows, owners * order), jnp.bfloat16),
            jax.ShapeDtypeStruct((1, order), jnp.float32),
            jax.ShapeDtypeStruct((1, order), jnp.float32),
        ),
        in_specs=[hbm] * 8,
        out_specs=(vmem, vmem, vmem),
        scratch_shapes=[
            pltpu.SMEM((1, owners), jnp.int32),
            pltpu.VMEM((owners, my_rows, order), jnp.bfloat16),
            pltpu.VMEM((1, order), jnp.float32),
            pltpu.VMEM((1, order), jnp.float32),
            pltpu.VMEM((2, order, order), jnp.bfloat16),
            pltpu.VMEM((2, order, order), jnp.bfloat16),
            pltpu.VMEM((owners, my_rows, order), jnp.bfloat16),
            pltpu.VMEM((order, order), jnp.bfloat16),
            pltpu.VMEM((owners, my_rows, order), jnp.bfloat16),
            pltpu.VMEM((owners, 8, 128), jnp.float32),
            pltpu.VMEM((groups, 8, 128), jnp.float32),
            pltpu.VMEM((2, 8, 128), jnp.float32),
            pltpu.VMEM((2, order, order), jnp.float32),
            pltpu.VMEM((2, order, order), jnp.bfloat16),
            pltpu.VMEM((2, order, order), jnp.bfloat16),
            pltpu.VMEM((2, order, order), jnp.float32),
            pltpu.VMEM((2, order, order), jnp.bfloat16),
            pltpu.VMEM((2, order, order), jnp.bfloat16),
            pltpu.VMEM((2, order, 4 * BLOCK), jnp.bfloat16),
            pltpu.VMEM((2, order, 2 * BLOCK), jnp.bfloat16),
            pltpu.VMEM((order, order), jnp.bfloat16),
            dma((owners + 7,)),
            dma((owners - 1,)),
            dma((owners - 1,)),
            dma((owners - 1,)),
            dma((owners - 1,)),
            dma((groups - 1,)),
            dma((groups - 1,)),
            dma((owners - 1,)),
            dma((owners - 1,)),
        ],
        compiler_params=pltpu.CompilerParams(
            collective_id=0, has_side_effects=True, vmem_limit_bytes=16 * 1024 * 1024 + 40 * order * order
        ),
        name="soap",
    )(
        *[pltpu.with_memory_space_constraint(v, pltpu.HBM) for v in (table, grad[0], left_stat[0, 0], right_stat[0, 0], left_basis[0, 0], right_basis[0, 0],
        row_moment[0], col_moment[0])]
    )
    update, row_next, col_next = pl.pallas_call(
        store_kernel,
        out_shape=tuple(jax.ShapeDtypeStruct(a.shape, a.dtype) for a in (update, row_next, col_next)),
        in_specs=[vmem] * 3,
        out_specs=[hbm] * 3,
        scratch_shapes=[dma((3,))],
        compiler_params=pltpu.CompilerParams(vmem_limit_bytes=4 * 1024 * 1024),
        name="store",
    )(update, row_next, col_next)
    return (update[None], row_next[None], col_next[None])


def solution(mesh):
    in_specs = (
        P("grp", "fsdp", None),
        P("grp", None),
        P("grp", "fsdp", None, None),
        P("grp", "fsdp", None, None),
        P("grp", "fsdp", None, None),
        P("grp", "fsdp", None, None),
        P("grp", "fsdp", None),
        P("grp", "fsdp", None),
    )
    out_specs = (P("grp", "fsdp", None), P("grp", "fsdp", None), P("grp", "fsdp", None))
    return jax.shard_map(shards, mesh=mesh, in_specs=in_specs, out_specs=out_specs, check_vma=False)
```

```python
import functools
import jax
import jax.numpy as jnp
from jax import lax
from jax.experimental import pallas as pl
from jax.experimental.pallas import tpu as pltpu
from jax.sharding import PartitionSpec as P

DECAY_STAT = 0.95
DECAY_MOMENT = 0.95
CLIP_RMS = 0.5
EPSILON = 1e-08
BLOCK = 64
TILE = 256
RATE = 28
PANELS = (8, 8, 16, 16, 16)
SUB = 8

NN = (((1,), (0,)), ((), ()))
NT = (((1,), (1,)), ((), ()))
TN = (((0,), (0,)), ((), ()))
MESH = pl.DeviceIdType.MESH


def mm(a, b, dims=NN):
    return lax.dot_general(a, b, dims, preferred_element_type=jnp.float32)


def split(a):
    high = a.astype(jnp.bfloat16)
    return high, (a - high.astype(jnp.float32)).astype(jnp.bfloat16)


def mm_split(a, b, dims=NN):
    return mm(a[0], b[0], dims) + (mm(a[0], b[1], dims) + mm(a[1], b[0], dims))


def spread(rows, column, sides):
    low, high = (jnp.broadcast_to(rows[:, j : j + 1], rows.shape) for j in (column, BLOCK + column))
    return jnp.where(sides[: rows.shape[0]], low, high)


def invert(pack, pump):
    shape = pack.shape
    lane = lax.broadcasted_iota(jnp.int32, shape, 1)
    row = lax.broadcasted_iota(jnp.int32, shape, 0)
    sides = lane < BLOCK
    local = jnp.where(sides, lane, lane - BLOCK)
    top = row[:SUB]
    done = []
    rest = pack
    start = 0
    for width in PANELS:
        columns = [spread(rest[q // SUB * SUB :], start + q, sides) for q in range(width)]
        here = local[: rest.shape[0]] - start
        unit = jnp.where(here == row[: rest.shape[0]], 1.0, 0.0)
        rest = jnp.where((here >= 0) & (here < width), unit, rest)
        for p in range(width):
            s = p % SUB
            column = columns[p]
            pivot = column[s : s + 1]
            inverse = 1.0 / pivot
            root = lax.rsqrt(pivot)
            scale = jnp.where(top == s, root, 1.0 if s == 0 else scale)
            raw = jnp.where(top > s, column[:SUB], 0.0)
            if column.shape[0] > SUB:
                raw = jnp.concatenate([raw, column[SUB:]], axis=0)
            factor = raw * inverse
            for q in range(p + 1, width):
                m = q - p + s
                skip = 0 if q // SUB == p // SUB else SUB
                taken = factor[skip:] * column[m : m + 1]
                if q == p + 1:
                    soon = raw[skip : skip + SUB] * column[m : m + 1] * inverse
                    taken = jnp.concatenate([soon, taken[SUB:]], axis=0) if taken.shape[0] > SUB else soon
                columns[q] = columns[q] - taken
            rest = rest - factor * rest[s : s + 1]
            if s == SUB - 1:
                done.append(rest[:SUB] * scale)
                rest = rest[SUB:]
            pump()
        start += width
    return jnp.where(local <= row, jnp.concatenate(done, axis=0), 0.0)


def twice(a):
    return jnp.concatenate([a, a], axis=1)


def swap(pieces):
    return [pieces[i ^ 1] for i in range(len(pieces))]


def orthonormalize(strip, x_ref, s_ref, xh_ref, xl_ref, o_ref, m_ref, q_ref, half_ref, g_ref, turned_ref):
    order = x_ref.shape[-1]
    blocks = order // BLOCK
    group = 2 * BLOCK
    lane = lax.broadcasted_iota(jnp.int32, (BLOCK, group), 1)
    first = lane < BLOCK
    queue = []
    last = blocks - 1

    credit = [0]

    def price(rows, depth, width, turned):
        tiles = -(-depth // TILE) * -(-width // TILE)
        return tiles * max(rows // 2, TILE // 2 if turned else TILE // 4) // 2

    def later(deadline, cost, task, *arguments):
        place = len(queue)
        while place and queue[place - 1][0] > deadline:
            place -= 1
        queue.insert(place, (deadline, cost, functools.partial(task, *arguments)))

    def run():
        _, cost, task = queue.pop(0)
        credit[0] -= cost
        task()

    def pump():
        credit[0] = credit[0] + RATE
        while queue and credit[0] >= 0:
            run()
        if not queue:
            credit[0] = 0

    def flush(deadline):
        while queue and queue[0][0] <= deadline:
            run()
        credit[0] = 0

    def gram_strip(c, start, stop):
        rows = pl.ds(start, stop - start)
        high, low = split(x_ref[c, rows, :])
        xh_ref[c, rows, :] = high
        xl_ref[c, rows, :] = low
        width = stop
        others = []
        for ref in (xh_ref, xl_ref):
            pieces = [ref[c, i * BLOCK : (i + 1) * BLOCK, :] for i in range(width // BLOCK)]
            others.append(jnp.concatenate(swap(pieces) if c else pieces, axis=0))
        s_ref[c, rows, :width] = mm_split((high, low), others, NT)

    def lanes_of(b):
        return slice(b // 2 * group, b // 2 * group + group)

    def packed(b, rows):
        pair = [s_ref[c, rows, lanes_of(b)] for c in range(2)]
        keep = lax.broadcasted_iota(jnp.int32, pair[0].shape, 1) < BLOCK
        return jnp.where(keep, pair[b % 2], pair[1 - b % 2])

    for c in range(2):
        strip(c, 0)
        gram_strip(c, 0, group)
    start = group
    while start < order:
        stop = min(start + (group if start == group else 2 * group), order)
        for c in range(2):
            for t in range(start // group, stop // group):
                later(min(start // group, 2), 2 * price(group, order, order, False), strip, c, t)
            later(min(start // group, 2), 3 * price(stop - start, order, stop, True), gram_strip, c, start, stop)
        start = stop
    pack = packed(0, pl.ds(0, BLOCK))
    for b in range(blocks):
        inverse = invert(pack, pump)
        flush(b)
        own = (first, ~first) if b % 2 == 0 else (~first, first)
        sides = [jnp.where(own[c], inverse, 0.0) for c in range(2)]
        weights = [split(jnp.concatenate([side, side], axis=0)) for side in sides]

        def panel(b, weights, start, stop):
            rows = pl.ds(start, stop - start)
            high, low = split(packed(b, rows))
            both = jnp.concatenate([high, low], axis=1)
            keep = lax.broadcasted_iota(jnp.int32, (stop - start, group), 1) < BLOCK
            outs = [mm(both, twice(weights[c][0]), NT) + mm(both[:, :group], weights[c][1], NT) for c in range(2)]
            for c in range(2):
                high, low = split(outs[c])
                o_ref[b % 2, c, rows, :] = jnp.concatenate([high, low], axis=1)
                mixed = jnp.where(keep, high.astype(jnp.float32), low.astype(jnp.float32)).astype(jnp.bfloat16)
                for i in range(start // BLOCK, stop // BLOCK):
                    place = (i ^ c) * BLOCK
                    m_ref[b % 2, c, place : place + BLOCK, :] = mixed[i * BLOCK - start : (i + 1) * BLOCK - start]

        def trail(b, c, start, stop):
            rows = pl.ds(start, stop - start)
            near = (b + 1) // 2 * group
            far = -(-stop // group) * group
            cut = slice(near, far)
            s_ref[c, rows, cut] = s_ref[c, rows, cut] - mm(o_ref[b % 2, c, rows, :], twice(m_ref[b % 2, c, near:far, :]), NT)

        def finish(b, c, doubled):
            rows = pl.ds(b * BLOCK, BLOCK)
            high, low = split(x_ref[c, rows, :])
            left = jnp.concatenate(split(doubled), axis=1)
            q = mm(left, jnp.concatenate([high, low, high, low], axis=0))
            high, low = split(q)
            q_ref[c, rows, :] = high
            xl_ref[c, rows, :] = low
            if c == 0:
                half_ref[rows, :] = mm(high, g_ref[...]).astype(jnp.bfloat16)

        def turn(t):
            rows = slice(t * group, (t + 1) * group)
            turned_ref[:, rows] = q_ref[0, rows, :].T

        def deflate(b, c, start, stop):
            rows = pl.ds(start, stop - start)
            done = pl.ds(b * BLOCK, BLOCK)
            high, low = q_ref[c, done, :], xl_ref[c, done, :]
            x_ref[c, rows, :] = x_ref[c, rows, :] - mm(o_ref[b % 2, c, rows, :], jnp.concatenate([high, low, high, low], axis=0))

        near = (b + 1) * BLOCK
        if near < order:
            if b % 2 == 0:
                for c in range(2):
                    place = (b ^ c) * BLOCK
                    m_ref[b % 2, c, place : place + BLOCK, :] = jnp.zeros((BLOCK, group), jnp.bfloat16)
            else:
                for c in range(2):
                    place = ((b + 2) ^ c) * BLOCK
                    m_ref[b % 2, c, place : place + BLOCK, :] = jnp.zeros((BLOCK, group), jnp.bfloat16)
            panel(b, weights, near, near + BLOCK)
            for c in range(2):
                trail(b, c, near, near + BLOCK)
            pack = packed(b + 1, pl.ds(near, BLOCK))
        rolled = pltpu.roll(inverse, BLOCK, 1)
        doubled = [jnp.where(own[c], inverse, rolled) for c in range(2)]
        chunks = []
        middle = min(order, (near + BLOCK) // group * group + group)
        for deadline, start, stop in ((b + 1, near + BLOCK, middle), (min(b + 2, last), middle, order)):
            if start < stop:
                chunks.append((deadline, start, stop))
        for deadline, start, stop in chunks:
            later(deadline, price(stop - start, 2 * TILE, TILE, True), panel, b, weights, start, stop)
            for c in range(2):
                later(deadline, price(stop - start, TILE, stop - near, True), trail, b, c, start, stop)
        for c in range(2):
            cost = price(BLOCK, TILE, order, False) + (price(BLOCK, order, order, False) if c == 0 else 0)
            later(min(b + 2, last), cost, finish, b, c, doubled[c])
        if b % 2:
            later(min(b + 2, last), 0, turn, b // 2)
        if near < order:
            for c in range(2):
                later(min(b + 2, last), price(order - near, TILE, order, False), deflate, b, c, near, order)
    flush(last)


def partners(owners):
    return [(chip, core) for chip in range(owners // 2 - 1, -1, -1) for core in (1, 0) if chip or core]


def soap_kernel(
    groups, table_hbm, grad_hbm, ls_hbm, rs_hbm, lb_hbm, rb_hbm, rm_hbm, cm_hbm, out_ref, rn_ref, cn_ref,
    table_ref, grad_ref, rm_ref, cm_ref,
    stat_ref, basis_ref, send_ref, block_ref, ret_ref, sums_ref, totals_ref, part_ref,
    x_ref, q_ref, turned_ref, s_ref, xh_ref, xl_ref, o_ref, m_ref, half_ref, spare_ref, rows_ref,
    load_sem, stripe_send, stripe_recv, sum_send, sum_recv, total_send, total_recv, slab_send, slab_recv,
):
    owners, my_rows, order = send_ref.shape
    me = lax.axis_index("fsdp")
    group = lax.axis_index("grp")
    offsets = partners(owners)

    def peer(offset):
        return lax.rem(me // 2 + offset[0], owners // 2) * 2 + lax.rem(me + offset[1], 2)

    def group_peer(step):
        return lax.rem(group + step, groups)

    loads = []

    def load(source, target):
        loads.append(pltpu.make_async_copy(source, target, load_sem.at[len(loads)]))
        loads[-1].start()
        return loads[-1]

    gradient = [load(table_hbm, table_ref)]
    for j in range(owners):
        gradient.append(load(grad_hbm.at[:, pl.ds(j * order, order)], grad_ref.at[j]))
    left = [load(lb_hbm, basis_ref.at[0]), load(ls_hbm, stat_ref.at[0])]
    right = [load(rb_hbm, basis_ref.at[1]), load(rs_hbm, stat_ref.at[1])]
    moments = [load(rm_hbm, rm_ref), load(cm_hbm, cm_ref)]
    barrier = pltpu.get_barrier_semaphore()
    for offset in offsets:
        pl.semaphore_signal(barrier, inc=1, device_id={"fsdp": peer(offset)}, device_id_type=MESH)
    for step in range(1, groups):
        pl.semaphore_signal(barrier, inc=1, device_id={"grp": group_peer(step)}, device_id_type=MESH)
    for copy in gradient:
        copy.wait()

    def stripe(owner):
        column = jnp.int32(0)
        for j in range(1, owners):
            column = jnp.where(table_ref[0, j] == owner, j, column)
        return grad_ref[column]

    for offset in offsets:
        owner = peer(offset)
        send_ref[owner] = stripe(owner)
    my_slab = pl.ds(pl.multiple_of(me * my_rows, my_rows), my_rows)
    block_ref[my_slab, :] = stripe(me)
    local = jnp.zeros((1, order), jnp.float32)
    for j in range(owners):
        piece = grad_ref[j].astype(jnp.float32)
        local = local + jnp.sum(piece * piece, axis=0, keepdims=True)
    local = jnp.broadcast_to(jnp.sum(local, axis=1, keepdims=True), sums_ref.shape[1:])
    part_ref[0] = local
    sums_ref[me] = local
    pl.semaphore_wait(barrier, owners - 1 + groups - 1)

    sum_copies, stripe_copies, total_copies, slab_copies = [], [], [], []
    for i, offset in enumerate(offsets):
        sum_copies.append(
            pltpu.make_async_remote_copy(
                src_ref=part_ref.at[0], dst_ref=sums_ref.at[me], send_sem=sum_send.at[i], recv_sem=sum_recv.at[i],
                device_id={"fsdp": peer(offset)}, device_id_type=MESH,
            )
        )
        sum_copies[-1].start()
    for i, offset in enumerate(offsets):
        stripe_copies.append(
            pltpu.make_async_remote_copy(
                src_ref=send_ref.at[peer(offset)], dst_ref=block_ref.at[my_slab, :],
                send_sem=stripe_send.at[i], recv_sem=stripe_recv.at[i],
                device_id={"fsdp": peer(offset)}, device_id_type=MESH,
            )
        )
        stripe_copies[-1].start()
    for copy in left:
        copy.wait()
    turned_ref[0] = basis_ref[0].T
    x_ref[0] = mm(turned_ref[0], stat_ref[0])
    for copy in sum_copies:
        copy.wait_recv()
    matrix_sum = sums_ref[0]
    for i in range(1, owners):
        matrix_sum = matrix_sum + sums_ref[i]
    part_ref[1] = matrix_sum
    totals_ref[group] = matrix_sum
    for copy in right:
        copy.wait()
    for copy in moments:
        copy.wait()
    for step in range(1, groups):
        total_copies.append(
            pltpu.make_async_remote_copy(
                src_ref=part_ref.at[1], dst_ref=totals_ref.at[group],
                send_sem=total_send.at[step - 1], recv_sem=total_recv.at[step - 1],
                device_id={"grp": group_peer(step)}, device_id_type=MESH,
            )
        )
        total_copies[-1].start()
    turned_ref[1] = basis_ref[1].T
    x_ref[1] = mm(turned_ref[1], stat_ref[1])
    rows_ref[...] = jnp.broadcast_to(rm_ref[...], (rows_ref.shape[1], order)).T
    for copy in stripe_copies:
        copy.wait_recv()
    g = block_ref[...]
    for c, dims in enumerate((NT, TN)):
        stat_ref[c], basis_ref[c] = split(mm(g, g, dims))
    for copy in total_copies:
        copy.wait_recv()
    total = totals_ref[0]
    for i in range(1, groups):
        total = total + totals_ref[i]
    count = float(groups * owners * order * order)
    clip = (CLIP_RMS / jnp.sqrt(total / count + 1e-06))[:1, :1]
    weight = (1.0 - DECAY_STAT) * clip * clip

    def strip(c, t):
        rows = pl.ds(t * 2 * BLOCK, 2 * BLOCK)
        left = turned_ref[c, rows, :]
        product = mm(left, stat_ref[c]) + mm(left, basis_ref[c])
        x_ref[c, rows, :] = DECAY_STAT * x_ref[c, rows, :] + weight * product

    orthonormalize(strip, x_ref, s_ref, xh_ref, xl_ref, o_ref, m_ref, q_ref, half_ref, block_ref, spare_ref)
    half = half_ref[...]
    rotated = clip * mm(half, q_ref[1], NT)
    square = rotated * rotated
    row_next = DECAY_MOMENT * rows_ref[...] + (1.0 - DECAY_MOMENT) * jnp.mean(square, axis=1, keepdims=True)
    col_next = DECAY_MOMENT * cm_ref[...] + (1.0 - DECAY_MOMENT) * jnp.mean(square, axis=0, keepdims=True)
    row_root = jnp.sqrt(row_next / jnp.mean(row_next, axis=0, keepdims=True))
    spread_root = jnp.concatenate([row_root] * (order // row_root.shape[1]), axis=1)
    normed = (rotated / (spread_root * jnp.sqrt(col_next) + EPSILON)).astype(jnp.bfloat16)
    for copy in stripe_copies:
        copy.wait_send()

    def back(owner):
        rows = pl.ds(pl.multiple_of(owner * my_rows, my_rows), my_rows)
        return mm(spare_ref[rows, :], normed).astype(jnp.bfloat16)

    targets = [peer(offset) for offset in offsets] + [me]
    turned = back(targets[0])
    for i, owner in enumerate(targets):
        slab = mm(turned, q_ref[1]).astype(jnp.bfloat16)
        if i == len(offsets):
            ret_ref[me] = slab
            break
        send_ref[owner] = slab
        turned = back(targets[i + 1])
        slab_copies.append(
            pltpu.make_async_remote_copy(
                src_ref=send_ref.at[owner], dst_ref=ret_ref.at[me],
                send_sem=slab_send.at[i], recv_sem=slab_recv.at[i],
                device_id={"fsdp": owner}, device_id_type=MESH,
            )
        )
        slab_copies[-1].start()
    rn_ref[...] = row_next.T[:1]
    cn_ref[...] = col_next
    for copy in slab_copies:
        copy.wait_recv()
    for j in range(owners):
        out_ref[:, j * order : (j + 1) * order] = ret_ref[table_ref[0, j]]
    for copy in sum_copies + total_copies + slab_copies:
        copy.wait_send()


def store_kernel(update_ref, rn_ref, cn_ref, update_hbm, rn_hbm, cn_hbm, sem):
    copies = [
        pltpu.make_async_copy(source, target, sem.at[i])
        for i, (source, target) in enumerate(((update_ref, update_hbm), (rn_ref, rn_hbm), (cn_ref, cn_hbm)))
    ]
    for copy in copies:
        copy.start()
    for copy in copies:
        copy.wait()


def shards(grad, table, left_stat, right_stat, left_basis, right_basis, row_moment, col_moment):
    order = left_stat.shape[-1]
    owners = lax.axis_size("fsdp")
    groups = lax.axis_size("grp")
    my_rows = grad.shape[1]
    vmem = pl.BlockSpec(memory_space=pltpu.VMEM)
    hbm = pl.BlockSpec(memory_space=pltpu.HBM)
    dma = pltpu.SemaphoreType.DMA
    update, row_next, col_next = pl.pallas_call(
        functools.partial(soap_kernel, groups),
        out_shape=(
            jax.ShapeDtypeStruct((my_rows, owners * order), jnp.bfloat16),
            jax.ShapeDtypeStruct((1, order), jnp.float32),
            jax.ShapeDtypeStruct((1, order), jnp.float32),
        ),
        in_specs=[hbm] * 8,
        out_specs=(vmem, vmem, vmem),
        scratch_shapes=[
            pltpu.SMEM((1, owners), jnp.int32),
            pltpu.VMEM((owners, my_rows, order), jnp.bfloat16),
            pltpu.VMEM((1, order), jnp.float32),
            pltpu.VMEM((1, order), jnp.float32),
            pltpu.VMEM((2, order, order), jnp.bfloat16),
            pltpu.VMEM((2, order, order), jnp.bfloat16),
            pltpu.VMEM((owners, my_rows, order), jnp.bfloat16),
            pltpu.VMEM((order, order), jnp.bfloat16),
            pltpu.VMEM((owners, my_rows, order), jnp.bfloat16),
            pltpu.VMEM((owners, 8, 128), jnp.float32),
            pltpu.VMEM((groups, 8, 128), jnp.float32),
            pltpu.VMEM((2, 8, 128), jnp.float32),
            pltpu.VMEM((2, order, order), jnp.float32),
            pltpu.VMEM((2, order, order), jnp.bfloat16),
            pltpu.VMEM((2, order, order), jnp.bfloat16),
            pltpu.VMEM((2, order, order), jnp.float32),
            pltpu.VMEM((2, order, order), jnp.bfloat16),
            pltpu.VMEM((2, order, order), jnp.bfloat16),
            pltpu.VMEM((2, 2, order, 4 * BLOCK), jnp.bfloat16),
            pltpu.VMEM((2, 2, order, 2 * BLOCK), jnp.bfloat16),
            pltpu.VMEM((order, order), jnp.bfloat16),
            pltpu.VMEM((order, order), jnp.bfloat16),
            pltpu.VMEM((order, 128), jnp.float32),
            dma((owners + 7,)),
            dma((owners - 1,)),
            dma((owners - 1,)),
            dma((owners - 1,)),
            dma((owners - 1,)),
            dma((groups - 1,)),
            dma((groups - 1,)),
            dma((owners - 1,)),
            dma((owners - 1,)),
        ],
        compiler_params=pltpu.CompilerParams(
            collective_id=0, has_side_effects=True, vmem_limit_bytes=16 * 1024 * 1024 + 40 * order * order
        ),
        name="soap",
    )(
        *[pltpu.with_memory_space_constraint(v, pltpu.HBM) for v in (table, grad[0], left_stat[0, 0], right_stat[0, 0], left_basis[0, 0], right_basis[0, 0],
        row_moment[0], col_moment[0])]
    )
    update, row_next, col_next = pl.pallas_call(
        store_kernel,
        out_shape=tuple(jax.ShapeDtypeStruct(a.shape, a.dtype) for a in (update, row_next, col_next)),
        in_specs=[vmem] * 3,
        out_specs=[hbm] * 3,
        scratch_shapes=[dma((3,))],
        compiler_params=pltpu.CompilerParams(vmem_limit_bytes=4 * 1024 * 1024),
        name="store",
    )(update, row_next, col_next)
    return (update[None], row_next[None], col_next[None])


def solution(mesh):
    in_specs = (
        P("grp", "fsdp", None),
        P("grp", None),
        P("grp", "fsdp", None, None),
        P("grp", "fsdp", None, None),
        P("grp", "fsdp", None, None),
        P("grp", "fsdp", None, None),
        P("grp", "fsdp", None),
        P("grp", "fsdp", None),
    )
    out_specs = (P("grp", "fsdp", None), P("grp", "fsdp", None), P("grp", "fsdp", None))
    return jax.shard_map(shards, mesh=mesh, in_specs=in_specs, out_specs=out_specs, check_vma=False)
```

```python
import functools
import jax
import jax.numpy as jnp
from jax import lax
from jax.experimental import pallas as pl
from jax.experimental.pallas import tpu as pltpu
from jax.sharding import PartitionSpec as P

DECAY_STAT = 0.95
DECAY_MOMENT = 0.95
CLIP_RMS = 0.5
EPSILON = 1e-08
BLOCK = 64
TILE = 256
RATE = 22
LAG = 3
PANELS = (8, 8, 8, 8, 16, 16)
SUB = 8

NN = (((1,), (0,)), ((), ()))
NT = (((1,), (1,)), ((), ()))
TN = (((0,), (0,)), ((), ()))
MESH = pl.DeviceIdType.MESH


def mm(a, b, dims=NN):
    return lax.dot_general(a, b, dims, preferred_element_type=jnp.float32)


def split(a):
    high = a.astype(jnp.bfloat16)
    return high, (a - high.astype(jnp.float32)).astype(jnp.bfloat16)


def mm_split(a, b, dims=NN):
    return mm(a[0], b[0], dims) + (mm(a[0], b[1], dims) + mm(a[1], b[0], dims))


def spread(rows, column, sides):
    low, high = (jnp.broadcast_to(rows[:, j : j + 1], rows.shape) for j in (column, BLOCK + column))
    return jnp.where(sides[: rows.shape[0]], low, high)


def invert(pack, pump):
    shape = pack.shape
    lane = lax.broadcasted_iota(jnp.int32, shape, 1)
    row = lax.broadcasted_iota(jnp.int32, shape, 0)
    sides = lane < BLOCK
    local = jnp.where(sides, lane, lane - BLOCK)
    top = row[:SUB]
    done = []
    rest = pack
    start = 0
    for width in PANELS:
        columns = [spread(rest[q // SUB * SUB :], start + q, sides) for q in range(width)]
        here = local[: rest.shape[0]] - start
        unit = jnp.where(here == row[: rest.shape[0]], 1.0, 0.0)
        rest = jnp.where((here >= 0) & (here < width), unit, rest)
        for p in range(width):
            s = p % SUB
            column = columns[p]
            pivot = column[s : s + 1]
            inverse = 1.0 / pivot
            root = lax.rsqrt(pivot)
            scale = jnp.where(top == s, root, 1.0 if s == 0 else scale)
            raw = jnp.where(top > s, column[:SUB], 0.0)
            if column.shape[0] > SUB:
                raw = jnp.concatenate([raw, column[SUB:]], axis=0)
            factor = raw * inverse
            for q in range(p + 1, width):
                m = q - p + s
                skip = 0 if q // SUB == p // SUB else SUB
                taken = factor[skip:] * column[m : m + 1]
                if q == p + 1:
                    soon = raw[skip : skip + SUB] * column[m : m + 1] * inverse
                    taken = jnp.concatenate([soon, taken[SUB:]], axis=0) if taken.shape[0] > SUB else soon
                columns[q] = columns[q] - taken
            rest = rest - factor * rest[s : s + 1]
            if s == SUB - 1:
                done.append(rest[:SUB] * scale)
                rest = rest[SUB:]
            pump()
        start += width
    return jnp.where(local <= row, jnp.concatenate(done, axis=0), 0.0)


def twice(a):
    return jnp.concatenate([a, a], axis=1)


def swap(pieces):
    return [pieces[i ^ 1] for i in range(len(pieces))]


def orthonormalize(strip, x_ref, s_ref, xh_ref, xl_ref, o_ref, m_ref, q_ref, half_ref, g_ref, turned_ref):
    order = x_ref.shape[-1]
    blocks = order // BLOCK
    group = 2 * BLOCK
    lane = lax.broadcasted_iota(jnp.int32, (BLOCK, group), 1)
    first = lane < BLOCK
    queue = []
    last = blocks - 1

    credit = [0]

    def price(rows, depth, width, turned):
        tiles = -(-depth // TILE) * -(-width // TILE)
        return tiles * max(rows // 2, TILE // 2 if turned else TILE // 4) // 2

    def later(deadline, cost, task, *arguments):
        place = len(queue)
        while place and queue[place - 1][0] > deadline:
            place -= 1
        queue.insert(place, (deadline, cost, functools.partial(task, *arguments)))

    def run():
        _, cost, task = queue.pop(0)
        credit[0] -= cost
        task()

    def pump():
        credit[0] = credit[0] + RATE
        while queue and credit[0] >= 0:
            run()
        if not queue:
            credit[0] = 0

    def flush(deadline):
        while queue and queue[0][0] <= deadline:
            run()
        credit[0] = 0

    def gram_strip(c, start, stop):
        rows = pl.ds(start, stop - start)
        high, low = split(x_ref[c, rows, :])
        xh_ref[c, rows, :] = high
        xl_ref[c, rows, :] = low
        width = stop
        others = []
        for ref in (xh_ref, xl_ref):
            pieces = [ref[c, i * BLOCK : (i + 1) * BLOCK, :] for i in range(width // BLOCK)]
            others.append(jnp.concatenate(swap(pieces) if c else pieces, axis=0))
        s_ref[c, rows, :width] = mm_split((high, low), others, NT)

    def lanes_of(b):
        return slice(b // 2 * group, b // 2 * group + group)

    def packed(b, rows):
        pair = [s_ref[c, rows, lanes_of(b)] for c in range(2)]
        keep = lax.broadcasted_iota(jnp.int32, pair[0].shape, 1) < BLOCK
        return jnp.where(keep, pair[b % 2], pair[1 - b % 2])

    for c in range(2):
        strip(c, 0, group)
        gram_strip(c, 0, group)
    start = group
    while start < order:
        stop = min(start + (group if start == group else 2 * group), order)
        for c in range(2):
            cost = price(stop - start, order, order, c == 1) + price(2 * (stop - start), order, order, c == 0)
            later(1 if start == group else min(LAG, last), cost, strip, c, start, stop)
            later(1 if start == group else min(LAG, last), 3 * price(stop - start, order, stop, True), gram_strip, c, start, stop)
        start = stop
    pack = packed(0, pl.ds(0, BLOCK))
    for b in range(blocks):
        inverse = invert(pack, pump)
        flush(b)
        own = (first, ~first) if b % 2 == 0 else (~first, first)
        sides = [jnp.where(own[c], inverse, 0.0) for c in range(2)]
        weights = [split(jnp.concatenate([side, side], axis=0)) for side in sides]

        def panel(b, weights, start, stop):
            rows = pl.ds(start, stop - start)
            high, low = split(packed(b, rows))
            both = jnp.concatenate([high, low], axis=1)
            keep = lax.broadcasted_iota(jnp.int32, (stop - start, group), 1) < BLOCK
            outs = [mm(both, twice(weights[c][0]), NT) + mm(both[:, :group], weights[c][1], NT) for c in range(2)]
            for c in range(2):
                high, low = split(outs[c])
                o_ref[b % LAG, c, rows, :] = jnp.concatenate([high, low], axis=1)
                mixed = jnp.where(keep, high.astype(jnp.float32), low.astype(jnp.float32)).astype(jnp.bfloat16)
                for i in range(start // BLOCK, stop // BLOCK):
                    place = (i ^ c) * BLOCK
                    m_ref[b % LAG, c, place : place + BLOCK, :] = mixed[i * BLOCK - start : (i + 1) * BLOCK - start]

        def trail(b, c, start, stop):
            rows = pl.ds(start, stop - start)
            near = (b + 1) // 2 * group
            far = -(-stop // group) * group
            cut = slice(near, far)
            s_ref[c, rows, cut] = s_ref[c, rows, cut] - mm(o_ref[b % LAG, c, rows, :], twice(m_ref[b % LAG, c, near:far, :]), NT)

        def finish(b, c, doubled):
            rows = pl.ds(b * BLOCK, BLOCK)
            high, low = split(x_ref[c, rows, :])
            left = jnp.concatenate(split(doubled), axis=1)
            q = mm(left, jnp.concatenate([high, low, high, low], axis=0))
            high, low = split(q)
            q_ref[c, rows, :] = high
            xl_ref[c, rows, :] = low
            if c == 0:
                half_ref[rows, :] = mm(high, g_ref[...]).astype(jnp.bfloat16)

        def turn(t):
            rows = slice(t * group, (t + 1) * group)
            turned_ref[:, rows] = q_ref[0, rows, :].T

        def deflate(b, c, start, stop):
            rows = pl.ds(start, stop - start)
            done = pl.ds(b * BLOCK, BLOCK)
            high, low = q_ref[c, done, :], xl_ref[c, done, :]
            x_ref[c, rows, :] = x_ref[c, rows, :] - mm(o_ref[b % LAG, c, rows, :], jnp.concatenate([high, low, high, low], axis=0))

        near = (b + 1) * BLOCK
        if near < order:
            if b % 2 == 0:
                for c in range(2):
                    place = (b ^ c) * BLOCK
                    m_ref[b % LAG, c, place : place + BLOCK, :] = jnp.zeros((BLOCK, group), jnp.bfloat16)
            else:
                for c in range(2):
                    place = ((b + 2) ^ c) * BLOCK
                    m_ref[b % LAG, c, place : place + BLOCK, :] = jnp.zeros((BLOCK, group), jnp.bfloat16)
            panel(b, weights, near, near + BLOCK)
            for c in range(2):
                trail(b, c, near, near + BLOCK)
            pack = packed(b + 1, pl.ds(near, BLOCK))
        rolled = pltpu.roll(inverse, BLOCK, 1)
        doubled = [jnp.where(own[c], inverse, rolled) for c in range(2)]
        chunks = []
        middle = min(order, (near + BLOCK) // group * group + group)
        due = min(b + LAG, max(b + 2, middle // BLOCK - 1), last)
        for deadline, start, stop in ((b + 1, near + BLOCK, middle), (due, middle, order)):
            if start < stop:
                chunks.append((deadline, start, stop))
        for deadline, start, stop in chunks:
            later(deadline, price(stop - start, 2 * TILE, TILE, True), panel, b, weights, start, stop)
            for c in range(2):
                later(deadline, price(stop - start, TILE, stop - near, True), trail, b, c, start, stop)
        for c in range(2):
            cost = price(BLOCK, TILE, order, False) + (price(BLOCK, order, order, False) if c == 0 else 0)
            later(min(b + LAG, last), cost, finish, b, c, doubled[c])
        if b % 2:
            later(min(b + LAG, last), 0, turn, b // 2)
        if near < order:
            for c in range(2):
                later(min(b + LAG, last), price(order - near, TILE, order, False), deflate, b, c, near, order)
    flush(last)


def partners(owners):
    return [(chip, core) for chip in range(owners // 2 - 1, -1, -1) for core in (1, 0) if chip or core]


def soap_kernel(
    groups, table_hbm, grad_hbm, ls_hbm, rs_hbm, lb_hbm, rb_hbm, rm_hbm, cm_hbm, out_ref, rn_ref, cn_ref,
    table_ref, grad_ref, rm_ref, cm_ref,
    stat_ref, basis_ref, send_ref, block_ref, ret_ref, sums_ref, totals_ref, part_ref,
    x_ref, q_ref, turned_ref, s_ref, xh_ref, xl_ref, o_ref, m_ref, half_ref, spare_ref, rows_ref,
    load_sem, stripe_send, stripe_recv, sum_send, sum_recv, total_send, total_recv, slab_send, slab_recv,
):
    owners, my_rows, order = send_ref.shape
    me = lax.axis_index("fsdp")
    group = lax.axis_index("grp")
    offsets = partners(owners)

    def peer(offset):
        return lax.rem(me // 2 + offset[0], owners // 2) * 2 + lax.rem(me + offset[1], 2)

    def group_peer(step):
        return lax.rem(group + step, groups)

    loads = []

    def load(source, target):
        loads.append(pltpu.make_async_copy(source, target, load_sem.at[len(loads)]))
        loads[-1].start()
        return loads[-1]

    gradient = [load(table_hbm, table_ref)]
    for j in range(owners):
        gradient.append(load(grad_hbm.at[:, pl.ds(j * order, order)], grad_ref.at[j]))
    left = [load(lb_hbm, basis_ref.at[0]), load(ls_hbm, stat_ref.at[0])]
    right = [load(rb_hbm, basis_ref.at[1]), load(rs_hbm, stat_ref.at[1])]
    moments = [load(rm_hbm, rm_ref), load(cm_hbm, cm_ref)]
    barrier = pltpu.get_barrier_semaphore()
    for offset in offsets:
        pl.semaphore_signal(barrier, inc=1, device_id={"fsdp": peer(offset)}, device_id_type=MESH)
    for step in range(1, groups):
        pl.semaphore_signal(barrier, inc=1, device_id={"grp": group_peer(step)}, device_id_type=MESH)
    for copy in gradient:
        copy.wait()

    def stripe(owner):
        column = jnp.int32(0)
        for j in range(1, owners):
            column = jnp.where(table_ref[0, j] == owner, j, column)
        return grad_ref[column]

    for offset in offsets:
        owner = peer(offset)
        send_ref[owner] = stripe(owner)
    my_slab = pl.ds(pl.multiple_of(me * my_rows, my_rows), my_rows)
    block_ref[my_slab, :] = stripe(me)
    local = jnp.zeros((1, order), jnp.float32)
    for j in range(owners):
        piece = grad_ref[j].astype(jnp.float32)
        local = local + jnp.sum(piece * piece, axis=0, keepdims=True)
    local = jnp.broadcast_to(jnp.sum(local, axis=1, keepdims=True), sums_ref.shape[1:])
    part_ref[0] = local
    sums_ref[me] = local
    pl.semaphore_wait(barrier, owners - 1 + groups - 1)

    sum_copies, stripe_copies, total_copies, slab_copies = [], [], [], []
    for i, offset in enumerate(offsets):
        sum_copies.append(
            pltpu.make_async_remote_copy(
                src_ref=part_ref.at[0], dst_ref=sums_ref.at[me], send_sem=sum_send.at[i], recv_sem=sum_recv.at[i],
                device_id={"fsdp": peer(offset)}, device_id_type=MESH,
            )
        )
        sum_copies[-1].start()
    for i, offset in enumerate(offsets):
        stripe_copies.append(
            pltpu.make_async_remote_copy(
                src_ref=send_ref.at[peer(offset)], dst_ref=block_ref.at[my_slab, :],
                send_sem=stripe_send.at[i], recv_sem=stripe_recv.at[i],
                device_id={"fsdp": peer(offset)}, device_id_type=MESH,
            )
        )
        stripe_copies[-1].start()
    for copy in left:
        copy.wait()
    turned_ref[0] = basis_ref[0].T
    x_ref[0] = mm(turned_ref[0], stat_ref[0])
    for copy in sum_copies:
        copy.wait_recv()
    matrix_sum = sums_ref[0]
    for i in range(1, owners):
        matrix_sum = matrix_sum + sums_ref[i]
    part_ref[1] = matrix_sum
    totals_ref[group] = matrix_sum
    for copy in right:
        copy.wait()
    for copy in moments:
        copy.wait()
    for step in range(1, groups):
        total_copies.append(
            pltpu.make_async_remote_copy(
                src_ref=part_ref.at[1], dst_ref=totals_ref.at[group],
                send_sem=total_send.at[step - 1], recv_sem=total_recv.at[step - 1],
                device_id={"grp": group_peer(step)}, device_id_type=MESH,
            )
        )
        total_copies[-1].start()
    turned_ref[1] = basis_ref[1].T
    x_ref[1] = mm(turned_ref[1], stat_ref[1])
    rows_ref[...] = jnp.broadcast_to(rm_ref[...], (rows_ref.shape[1], order)).T
    for copy in stripe_copies:
        copy.wait_recv()
    g = block_ref[...]

    def inner(c, start, stop):
        rows = pl.ds(start, stop - start)
        through = split(mm(turned_ref[c, rows, :], g, NT if c else NN))
        product = mm(jnp.concatenate(through, axis=0), g, NN if c else NT)
        return product[: stop - start] + product[stop - start :]

    heads = [inner(c, 0, 2 * BLOCK) for c in range(2)]
    for copy in total_copies:
        copy.wait_recv()
    total = totals_ref[0]
    for i in range(1, groups):
        total = total + totals_ref[i]
    count = float(groups * owners * order * order)
    clip = (CLIP_RMS / jnp.sqrt(total / count + 1e-06))[:1, :1]
    weight = (1.0 - DECAY_STAT) * clip * clip

    def strip(c, start, stop):
        rows = pl.ds(start, stop - start)
        product = inner(c, start, stop) if start else heads[c]
        x_ref[c, rows, :] = DECAY_STAT * x_ref[c, rows, :] + weight * product

    orthonormalize(strip, x_ref, s_ref, xh_ref, xl_ref, o_ref, m_ref, q_ref, half_ref, block_ref, spare_ref)
    half = half_ref[...]
    rotated = clip * mm(half, q_ref[1], NT)
    square = rotated * rotated
    row_next = DECAY_MOMENT * rows_ref[...] + (1.0 - DECAY_MOMENT) * jnp.mean(square, axis=1, keepdims=True)
    col_next = DECAY_MOMENT * cm_ref[...] + (1.0 - DECAY_MOMENT) * jnp.mean(square, axis=0, keepdims=True)
    row_root = jnp.sqrt(row_next / jnp.mean(row_next, axis=0, keepdims=True))
    spread_root = jnp.concatenate([row_root] * (order // row_root.shape[1]), axis=1)
    normed = (rotated / (spread_root * jnp.sqrt(col_next) + EPSILON)).astype(jnp.bfloat16)
    for copy in stripe_copies:
        copy.wait_send()

    def back(owner):
        rows = pl.ds(pl.multiple_of(owner * my_rows, my_rows), my_rows)
        return mm(spare_ref[rows, :], normed).astype(jnp.bfloat16)

    targets = [peer(offset) for offset in offsets] + [me]
    turned = back(targets[0])
    for i, owner in enumerate(targets):
        slab = mm(turned, q_ref[1]).astype(jnp.bfloat16)
        if i == len(offsets):
            ret_ref[me] = slab
            break
        send_ref[owner] = slab
        turned = back(targets[i + 1])
        slab_copies.append(
            pltpu.make_async_remote_copy(
                src_ref=send_ref.at[owner], dst_ref=ret_ref.at[me],
                send_sem=slab_send.at[i], recv_sem=slab_recv.at[i],
                device_id={"fsdp": owner}, device_id_type=MESH,
            )
        )
        slab_copies[-1].start()
    rn_ref[...] = row_next.T[:1]
    cn_ref[...] = col_next
    for copy in slab_copies:
        copy.wait_recv()
    for j in range(owners):
        out_ref[:, j * order : (j + 1) * order] = ret_ref[table_ref[0, j]]
    for copy in sum_copies + total_copies + slab_copies:
        copy.wait_send()


def store_kernel(update_ref, rn_ref, cn_ref, update_hbm, rn_hbm, cn_hbm, sem):
    copies = [
        pltpu.make_async_copy(source, target, sem.at[i])
        for i, (source, target) in enumerate(((update_ref, update_hbm), (rn_ref, rn_hbm), (cn_ref, cn_hbm)))
    ]
    for copy in copies:
        copy.start()
    for copy in copies:
        copy.wait()


def shards(grad, table, left_stat, right_stat, left_basis, right_basis, row_moment, col_moment):
    order = left_stat.shape[-1]
    owners = lax.axis_size("fsdp")
    groups = lax.axis_size("grp")
    my_rows = grad.shape[1]
    vmem = pl.BlockSpec(memory_space=pltpu.VMEM)
    hbm = pl.BlockSpec(memory_space=pltpu.HBM)
    dma = pltpu.SemaphoreType.DMA
    update, row_next, col_next = pl.pallas_call(
        functools.partial(soap_kernel, groups),
        out_shape=(
            jax.ShapeDtypeStruct((my_rows, owners * order), jnp.bfloat16),
            jax.ShapeDtypeStruct((1, order), jnp.float32),
            jax.ShapeDtypeStruct((1, order), jnp.float32),
        ),
        in_specs=[hbm] * 8,
        out_specs=(vmem, vmem, vmem),
        scratch_shapes=[
            pltpu.SMEM((1, owners), jnp.int32),
            pltpu.VMEM((owners, my_rows, order), jnp.bfloat16),
            pltpu.VMEM((1, order), jnp.float32),
            pltpu.VMEM((1, order), jnp.float32),
            pltpu.VMEM((2, order, order), jnp.bfloat16),
            pltpu.VMEM((2, order, order), jnp.bfloat16),
            pltpu.VMEM((owners, my_rows, order), jnp.bfloat16),
            pltpu.VMEM((order, order), jnp.bfloat16),
            pltpu.VMEM((owners, my_rows, order), jnp.bfloat16),
            pltpu.VMEM((owners, 8, 128), jnp.float32),
            pltpu.VMEM((groups, 8, 128), jnp.float32),
            pltpu.VMEM((2, 8, 128), jnp.float32),
            pltpu.VMEM((2, order, order), jnp.float32),
            pltpu.VMEM((2, order, order), jnp.bfloat16),
            pltpu.VMEM((2, order, order), jnp.bfloat16),
            pltpu.VMEM((2, order, order), jnp.float32),
            pltpu.VMEM((2, order, order), jnp.bfloat16),
            pltpu.VMEM((2, order, order), jnp.bfloat16),
            pltpu.VMEM((LAG, 2, order, 4 * BLOCK), jnp.bfloat16),
            pltpu.VMEM((LAG, 2, order, 2 * BLOCK), jnp.bfloat16),
            pltpu.VMEM((order, order), jnp.bfloat16),
            pltpu.VMEM((order, order), jnp.bfloat16),
            pltpu.VMEM((order, 128), jnp.float32),
            dma((owners + 7,)),
            dma((owners - 1,)),
            dma((owners - 1,)),
            dma((owners - 1,)),
            dma((owners - 1,)),
            dma((groups - 1,)),
            dma((groups - 1,)),
            dma((owners - 1,)),
            dma((owners - 1,)),
        ],
        compiler_params=pltpu.CompilerParams(
            collective_id=0, has_side_effects=True, vmem_limit_bytes=16 * 1024 * 1024 + 40 * order * order
        ),
        name="soap",
    )(
        *[pltpu.with_memory_space_constraint(v, pltpu.HBM) for v in (table, grad[0], left_stat[0, 0], right_stat[0, 0], left_basis[0, 0], right_basis[0, 0],
        row_moment[0], col_moment[0])]
    )
    update, row_next, col_next = pl.pallas_call(
        store_kernel,
        out_shape=tuple(jax.ShapeDtypeStruct(a.shape, a.dtype) for a in (update, row_next, col_next)),
        in_specs=[vmem] * 3,
        out_specs=[hbm] * 3,
        scratch_shapes=[dma((3,))],
        compiler_params=pltpu.CompilerParams(vmem_limit_bytes=4 * 1024 * 1024),
        name="store",
    )(update, row_next, col_next)
    return (update[None], row_next[None], col_next[None])


def solution(mesh):
    in_specs = (
        P("grp", "fsdp", None),
        P("grp", None),
        P("grp", "fsdp", None, None),
        P("grp", "fsdp", None, None),
        P("grp", "fsdp", None, None),
        P("grp", "fsdp", None, None),
        P("grp", "fsdp", None),
        P("grp", "fsdp", None),
    )
    out_specs = (P("grp", "fsdp", None), P("grp", "fsdp", None), P("grp", "fsdp", None))
    return jax.shard_map(shards, mesh=mesh, in_specs=in_specs, out_specs=out_specs, check_vma=False)
```

```python
import functools
import jax
import jax.numpy as jnp
from jax import lax
from jax.experimental import pallas as pl
from jax.experimental.pallas import tpu as pltpu
from jax.sharding import PartitionSpec as P

DECAY_STAT = 0.95
DECAY_MOMENT = 0.95
CLIP_RMS = 0.5
EPSILON = 1e-08
BLOCK = 64
TILE = 256
RATE = 20
LAG = 3
PANELS = (8, 8, 8, 8, 16, 16)
SUB = 8

NN = (((1,), (0,)), ((), ()))
NT = (((1,), (1,)), ((), ()))
TN = (((0,), (0,)), ((), ()))
MESH = pl.DeviceIdType.MESH


def mm(a, b, dims=NN):
    return lax.dot_general(a, b, dims, preferred_element_type=jnp.float32)


def split(a):
    high = a.astype(jnp.bfloat16)
    return high, (a - high.astype(jnp.float32)).astype(jnp.bfloat16)


def mm_split(a, b, dims=NN):
    return mm(a[0], b[0], dims) + (mm(a[0], b[1], dims) + mm(a[1], b[0], dims))


def spread(rows, column, sides):
    low, high = (jnp.broadcast_to(rows[:, j : j + 1], rows.shape) for j in (column, BLOCK + column))
    return jnp.where(sides[: rows.shape[0]], low, high)


def invert(pack, pump):
    shape = pack.shape
    lane = lax.broadcasted_iota(jnp.int32, shape, 1)
    row = lax.broadcasted_iota(jnp.int32, shape, 0)
    sides = lane < BLOCK
    local = jnp.where(sides, lane, lane - BLOCK)
    top = row[:SUB]
    done = []
    rest = pack
    start = 0
    for width in PANELS:
        columns = [spread(rest[q // SUB * SUB :], start + q, sides) for q in range(width)]
        here = local[: rest.shape[0]] - start
        unit = jnp.where(here == row[: rest.shape[0]], 1.0, 0.0)
        rest = jnp.where((here >= 0) & (here < width), unit, rest)
        for p in range(width):
            s = p % SUB
            column = columns[p]
            pivot = column[s : s + 1]
            inverse = 1.0 / pivot
            root = lax.rsqrt(pivot)
            scale = jnp.where(top == s, root, 1.0 if s == 0 else scale)
            raw = jnp.where(top > s, column[:SUB], 0.0)
            if column.shape[0] > SUB:
                raw = jnp.concatenate([raw, column[SUB:]], axis=0)
            factor = raw * inverse
            for q in range(p + 1, width):
                m = q - p + s
                skip = 0 if q // SUB == p // SUB else SUB
                taken = factor[skip:] * column[m : m + 1]
                if q == p + 1:
                    soon = raw[skip : skip + SUB] * column[m : m + 1] * inverse
                    taken = jnp.concatenate([soon, taken[SUB:]], axis=0) if taken.shape[0] > SUB else soon
                columns[q] = columns[q] - taken
            rest = rest - factor * rest[s : s + 1]
            if s == SUB - 1:
                done.append(rest[:SUB] * scale)
                rest = rest[SUB:]
            pump()
        start += width
    return jnp.where(local <= row, jnp.concatenate(done, axis=0), 0.0)


def twice(a):
    return jnp.concatenate([a, a], axis=1)


def swap(pieces):
    return [pieces[i ^ 1] for i in range(len(pieces))]


def orthonormalize(strip, x_ref, s_ref, xh_ref, xl_ref, o_ref, m_ref, q_ref, half_ref, g_ref, turned_ref):
    order = x_ref.shape[-1]
    blocks = order // BLOCK
    group = 2 * BLOCK
    lane = lax.broadcasted_iota(jnp.int32, (BLOCK, group), 1)
    first = lane < BLOCK
    queue = []
    last = blocks - 1

    credit = [0]

    def price(rows, depth, width, turned):
        tiles = -(-depth // TILE) * -(-width // TILE)
        return tiles * max(rows // 2, TILE // 2 if turned else TILE // 4) // 2

    def later(deadline, cost, task, *arguments):
        place = len(queue)
        while place and queue[place - 1][0] > deadline:
            place -= 1
        queue.insert(place, (deadline, cost, functools.partial(task, *arguments)))

    def run():
        _, cost, task = queue.pop(0)
        credit[0] -= cost
        task()

    def pump():
        credit[0] = credit[0] + RATE
        while queue and credit[0] >= 0:
            run()
        if not queue:
            credit[0] = 0

    def flush(deadline):
        while queue and queue[0][0] <= deadline:
            run()
        credit[0] = 0

    def gram_strip(c, start, stop):
        rows = pl.ds(start, stop - start)
        high, low = split(x_ref[c, rows, :])
        xh_ref[c, rows, :] = high
        xl_ref[c, rows, :] = low
        width = stop
        others = []
        for ref in (xh_ref, xl_ref):
            pieces = [ref[c, i * BLOCK : (i + 1) * BLOCK, :] for i in range(width // BLOCK)]
            others.append(jnp.concatenate(swap(pieces) if c else pieces, axis=0))
        s_ref[c, rows, :width] = mm_split((high, low), others, NT)

    def lanes_of(b):
        return slice(b // 2 * group, b // 2 * group + group)

    def packed(b, rows):
        pair = [s_ref[c, rows, lanes_of(b)] for c in range(2)]
        keep = lax.broadcasted_iota(jnp.int32, pair[0].shape, 1) < BLOCK
        return jnp.where(keep, pair[b % 2], pair[1 - b % 2])

    for c in range(2):
        strip(c, 0, group)
        gram_strip(c, 0, group)
    start = group
    while start < order:
        stop = min(start + (group if start == group else 2 * group), order)
        for c in range(2):
            cost = price(stop - start, order, order, c == 1) + price(2 * (stop - start), order, order, c == 0)
            later(1 if start == group else min(LAG, last), cost, strip, c, start, stop)
            later(1 if start == group else min(LAG, last), 3 * price(stop - start, order, stop, True), gram_strip, c, start, stop)
        start = stop
    pack = packed(0, pl.ds(0, BLOCK))
    for b in range(blocks):
        inverse = invert(pack, pump)
        flush(b)
        own = (first, ~first) if b % 2 == 0 else (~first, first)
        sides = [jnp.where(own[c], inverse, 0.0) for c in range(2)]
        weights = [split(jnp.concatenate([side, side], axis=0)) for side in sides]

        def panel(b, weights, start, stop):
            rows = pl.ds(start, stop - start)
            high, low = split(packed(b, rows))
            both = jnp.concatenate([high, low], axis=1)
            keep = lax.broadcasted_iota(jnp.int32, (stop - start, group), 1) < BLOCK
            outs = [mm(both, twice(weights[c][0]), NT) + mm(both[:, :group], weights[c][1], NT) for c in range(2)]
            for c in range(2):
                high, low = split(outs[c])
                o_ref[b % LAG, c, rows, :] = jnp.concatenate([high, low], axis=1)
                mixed = jnp.where(keep, high.astype(jnp.float32), low.astype(jnp.float32)).astype(jnp.bfloat16)
                for i in range(start // BLOCK, stop // BLOCK):
                    place = (i ^ c) * BLOCK
                    m_ref[b % LAG, c, place : place + BLOCK, :] = mixed[i * BLOCK - start : (i + 1) * BLOCK - start]

        def trail(b, c, start, stop):
            rows = pl.ds(start, stop - start)
            near = (b + 1) // 2 * group
            far = -(-stop // group) * group
            cut = slice(near, far)
            s_ref[c, rows, cut] = s_ref[c, rows, cut] - mm(o_ref[b % LAG, c, rows, :], twice(m_ref[b % LAG, c, near:far, :]), NT)

        def finish(b, c, doubled):
            rows = pl.ds(b * BLOCK, BLOCK)
            high, low = split(x_ref[c, rows, :])
            left = jnp.concatenate(split(doubled), axis=1)
            q = mm(left, jnp.concatenate([high, low, high, low], axis=0))
            high, low = split(q)
            q_ref[c, rows, :] = high
            xl_ref[c, rows, :] = low
            if c == 0:
                half_ref[rows, :] = mm(high, g_ref[...]).astype(jnp.bfloat16)

        def turn(t):
            rows = slice(t * group, (t + 1) * group)
            turned_ref[:, rows] = q_ref[0, rows, :].T

        def deflate(b, c, start, stop):
            rows = pl.ds(start, stop - start)
            done = pl.ds(b * BLOCK, BLOCK)
            high, low = q_ref[c, done, :], xl_ref[c, done, :]
            x_ref[c, rows, :] = x_ref[c, rows, :] - mm(o_ref[b % LAG, c, rows, :], jnp.concatenate([high, low, high, low], axis=0))

        near = (b + 1) * BLOCK
        if near < order:
            if b % 2 == 0:
                for c in range(2):
                    place = (b ^ c) * BLOCK
                    m_ref[b % LAG, c, place : place + BLOCK, :] = jnp.zeros((BLOCK, group), jnp.bfloat16)
            else:
                for c in range(2):
                    place = ((b + 2) ^ c) * BLOCK
                    m_ref[b % LAG, c, place : place + BLOCK, :] = jnp.zeros((BLOCK, group), jnp.bfloat16)
            panel(b, weights, near, near + BLOCK)
            for c in range(2):
                trail(b, c, near, near + BLOCK)
            pack = packed(b + 1, pl.ds(near, BLOCK))
        rolled = pltpu.roll(inverse, BLOCK, 1)
        doubled = [jnp.where(own[c], inverse, rolled) for c in range(2)]
        chunks = []
        middle = min(order, (near + BLOCK) // group * group + group)
        due = min(b + LAG, max(b + 2, middle // BLOCK - 1), last)
        for deadline, start, stop in ((b + 1, near + BLOCK, middle), (due, middle, order)):
            if start < stop:
                chunks.append((deadline, start, stop))
        for deadline, start, stop in chunks:
            later(deadline, price(stop - start, 2 * TILE, TILE, True), panel, b, weights, start, stop)
            for c in range(2):
                later(deadline, price(stop - start, TILE, stop - near, True), trail, b, c, start, stop)
        for c in range(2):
            cost = price(BLOCK, TILE, order, False) + (price(BLOCK, order, order, False) if c == 0 else 0)
            later(min(b + LAG, last), cost, finish, b, c, doubled[c])
        if b % 2:
            later(min(b + LAG, last), 0, turn, b // 2)
        if near < order:
            for c in range(2):
                later(min(b + LAG, last), price(order - near, TILE, order, False), deflate, b, c, near, order)
    flush(last)


def partners(owners):
    return [(chip, core) for chip in range(owners // 2 - 1, -1, -1) for core in (1, 0) if chip or core]


def soap_kernel(
    groups, table_hbm, grad_hbm, ls_hbm, rs_hbm, lb_hbm, rb_hbm, rm_hbm, cm_hbm, out_ref, rn_ref, cn_ref,
    table_ref, grad_ref, rm_ref, cm_ref,
    stat_ref, basis_ref, send_ref, block_ref, ret_ref, sums_ref, totals_ref, part_ref,
    x_ref, q_ref, turned_ref, s_ref, xh_ref, xl_ref, o_ref, m_ref, half_ref, spare_ref, rows_ref,
    load_sem, stripe_send, stripe_recv, sum_send, sum_recv, total_send, total_recv, slab_send, slab_recv,
):
    owners, my_rows, order = send_ref.shape
    me = lax.axis_index("fsdp")
    group = lax.axis_index("grp")
    offsets = partners(owners)

    def peer(offset):
        return lax.rem(me // 2 + offset[0], owners // 2) * 2 + lax.rem(me + offset[1], 2)

    def group_peer(step):
        return lax.rem(group + step, groups)

    loads = []

    def load(source, target):
        loads.append(pltpu.make_async_copy(source, target, load_sem.at[len(loads)]))
        loads[-1].start()
        return loads[-1]

    gradient = [load(table_hbm, table_ref)]
    for j in range(owners):
        gradient.append(load(grad_hbm.at[:, pl.ds(j * order, order)], grad_ref.at[j]))
    left = [load(lb_hbm, basis_ref.at[0]), load(ls_hbm, stat_ref.at[0])]
    right = [load(rb_hbm, basis_ref.at[1]), load(rs_hbm, stat_ref.at[1])]
    moments = [load(rm_hbm, rm_ref), load(cm_hbm, cm_ref)]
    barrier = pltpu.get_barrier_semaphore()
    for offset in offsets:
        pl.semaphore_signal(barrier, inc=1, device_id={"fsdp": peer(offset)}, device_id_type=MESH)
    for step in range(1, groups):
        pl.semaphore_signal(barrier, inc=1, device_id={"grp": group_peer(step)}, device_id_type=MESH)
    for copy in gradient:
        copy.wait()

    def stripe(owner):
        column = jnp.int32(0)
        for j in range(1, owners):
            column = jnp.where(table_ref[0, j] == owner, j, column)
        return grad_ref[column]

    for offset in offsets:
        owner = peer(offset)
        send_ref[owner] = stripe(owner)
    my_slab = pl.ds(pl.multiple_of(me * my_rows, my_rows), my_rows)
    block_ref[my_slab, :] = stripe(me)
    local = jnp.zeros((1, order), jnp.float32)
    for j in range(owners):
        piece = grad_ref[j].astype(jnp.float32)
        local = local + jnp.sum(piece * piece, axis=0, keepdims=True)
    local = jnp.broadcast_to(jnp.sum(local, axis=1, keepdims=True), sums_ref.shape[1:])
    part_ref[0] = local
    sums_ref[me] = local
    pl.semaphore_wait(barrier, owners - 1 + groups - 1)

    sum_copies, stripe_copies, total_copies, slab_copies = [], [], [], []
    for i, offset in enumerate(offsets):
        sum_copies.append(
            pltpu.make_async_remote_copy(
                src_ref=part_ref.at[0], dst_ref=sums_ref.at[me], send_sem=sum_send.at[i], recv_sem=sum_recv.at[i],
                device_id={"fsdp": peer(offset)}, device_id_type=MESH,
            )
        )
        sum_copies[-1].start()
    for i, offset in enumerate(offsets):
        stripe_copies.append(
            pltpu.make_async_remote_copy(
                src_ref=send_ref.at[peer(offset)], dst_ref=block_ref.at[my_slab, :],
                send_sem=stripe_send.at[i], recv_sem=stripe_recv.at[i],
                device_id={"fsdp": peer(offset)}, device_id_type=MESH,
            )
        )
        stripe_copies[-1].start()
    for copy in left:
        copy.wait()
    turned_ref[0] = basis_ref[0].T
    x_ref[0] = mm(turned_ref[0], stat_ref[0])
    for copy in sum_copies:
        copy.wait_recv()
    matrix_sum = sums_ref[0]
    for i in range(1, owners):
        matrix_sum = matrix_sum + sums_ref[i]
    part_ref[1] = matrix_sum
    totals_ref[group] = matrix_sum
    for copy in right:
        copy.wait()
    for copy in moments:
        copy.wait()
    for step in range(1, groups):
        total_copies.append(
            pltpu.make_async_remote_copy(
                src_ref=part_ref.at[1], dst_ref=totals_ref.at[group],
                send_sem=total_send.at[step - 1], recv_sem=total_recv.at[step - 1],
                device_id={"grp": group_peer(step)}, device_id_type=MESH,
            )
        )
        total_copies[-1].start()
    turned_ref[1] = basis_ref[1].T
    x_ref[1] = mm(turned_ref[1], stat_ref[1])
    rows_ref[...] = jnp.broadcast_to(rm_ref[...], (rows_ref.shape[1], order)).T
    for copy in stripe_copies:
        copy.wait_recv()
    g = block_ref[...]

    def inner(c, start, stop):
        rows = pl.ds(start, stop - start)
        through = split(mm(turned_ref[c, rows, :], g, NT if c else NN))
        product = mm(jnp.concatenate(through, axis=0), g, NN if c else NT)
        return product[: stop - start] + product[stop - start :]

    heads = [inner(c, 0, 2 * BLOCK) for c in range(2)]
    for copy in total_copies:
        copy.wait_recv()
    total = totals_ref[0]
    for i in range(1, groups):
        total = total + totals_ref[i]
    count = float(groups * owners * order * order)
    clip = (CLIP_RMS / jnp.sqrt(total / count + 1e-06))[:1, :1]
    weight = (1.0 - DECAY_STAT) * clip * clip

    def strip(c, start, stop):
        rows = pl.ds(start, stop - start)
        product = inner(c, start, stop) if start else heads[c]
        x_ref[c, rows, :] = DECAY_STAT * x_ref[c, rows, :] + weight * product

    orthonormalize(strip, x_ref, s_ref, xh_ref, xl_ref, o_ref, m_ref, q_ref, half_ref, block_ref, spare_ref)
    half = half_ref[...]
    rotated = clip * mm(half, q_ref[1], NT)
    square = rotated * rotated
    row_next = DECAY_MOMENT * rows_ref[...] + (1.0 - DECAY_MOMENT) * jnp.mean(square, axis=1, keepdims=True)
    col_next = DECAY_MOMENT * cm_ref[...] + (1.0 - DECAY_MOMENT) * jnp.mean(square, axis=0, keepdims=True)
    row_root = jnp.sqrt(row_next / jnp.mean(row_next, axis=0, keepdims=True))
    spread_root = jnp.concatenate([row_root] * (order // row_root.shape[1]), axis=1)
    normed = (rotated / (spread_root * jnp.sqrt(col_next) + EPSILON)).astype(jnp.bfloat16)
    for copy in stripe_copies:
        copy.wait_send()

    def back(owner):
        rows = pl.ds(pl.multiple_of(owner * my_rows, my_rows), my_rows)
        return mm(spare_ref[rows, :], normed).astype(jnp.bfloat16)

    targets = [peer(offset) for offset in offsets] + [me]
    turned = back(targets[0])
    for i, owner in enumerate(targets):
        slab = mm(turned, q_ref[1]).astype(jnp.bfloat16)
        if i == len(offsets):
            ret_ref[me] = slab
            break
        send_ref[owner] = slab
        turned = back(targets[i + 1])
        slab_copies.append(
            pltpu.make_async_remote_copy(
                src_ref=send_ref.at[owner], dst_ref=ret_ref.at[me],
                send_sem=slab_send.at[i], recv_sem=slab_recv.at[i],
                device_id={"fsdp": owner}, device_id_type=MESH,
            )
        )
        slab_copies[-1].start()
    rn_ref[...] = row_next.T[:1]
    cn_ref[...] = col_next
    for copy in slab_copies:
        copy.wait_recv()
    for j in range(owners):
        out_ref[:, j * order : (j + 1) * order] = ret_ref[table_ref[0, j]]
    for copy in sum_copies + total_copies + slab_copies:
        copy.wait_send()


def store_kernel(update_ref, rn_ref, cn_ref, update_hbm, rn_hbm, cn_hbm, sem):
    copies = [
        pltpu.make_async_copy(source, target, sem.at[i])
        for i, (source, target) in enumerate(((update_ref, update_hbm), (rn_ref, rn_hbm), (cn_ref, cn_hbm)))
    ]
    for copy in copies:
        copy.start()
    for copy in copies:
        copy.wait()


def shards(grad, table, left_stat, right_stat, left_basis, right_basis, row_moment, col_moment):
    order = left_stat.shape[-1]
    owners = lax.axis_size("fsdp")
    groups = lax.axis_size("grp")
    my_rows = grad.shape[1]
    vmem = pl.BlockSpec(memory_space=pltpu.VMEM)
    hbm = pl.BlockSpec(memory_space=pltpu.HBM)
    dma = pltpu.SemaphoreType.DMA
    update, row_next, col_next = pl.pallas_call(
        functools.partial(soap_kernel, groups),
        out_shape=(
            jax.ShapeDtypeStruct((my_rows, owners * order), jnp.bfloat16),
            jax.ShapeDtypeStruct((1, order), jnp.float32),
            jax.ShapeDtypeStruct((1, order), jnp.float32),
        ),
        in_specs=[hbm] * 8,
        out_specs=(vmem, vmem, vmem),
        scratch_shapes=[
            pltpu.SMEM((1, owners), jnp.int32),
            pltpu.VMEM((owners, my_rows, order), jnp.bfloat16),
            pltpu.VMEM((1, order), jnp.float32),
            pltpu.VMEM((1, order), jnp.float32),
            pltpu.VMEM((2, order, order), jnp.bfloat16),
            pltpu.VMEM((2, order, order), jnp.bfloat16),
            pltpu.VMEM((owners, my_rows, order), jnp.bfloat16),
            pltpu.VMEM((order, order), jnp.bfloat16),
            pltpu.VMEM((owners, my_rows, order), jnp.bfloat16),
            pltpu.VMEM((owners, 8, 128), jnp.float32),
            pltpu.VMEM((groups, 8, 128), jnp.float32),
            pltpu.VMEM((2, 8, 128), jnp.float32),
            pltpu.VMEM((2, order, order), jnp.float32),
            pltpu.VMEM((2, order, order), jnp.bfloat16),
            pltpu.VMEM((2, order, order), jnp.bfloat16),
            pltpu.VMEM((2, order, order), jnp.float32),
            pltpu.VMEM((2, order, order), jnp.bfloat16),
            pltpu.VMEM((2, order, order), jnp.bfloat16),
            pltpu.VMEM((LAG, 2, order, 4 * BLOCK), jnp.bfloat16),
            pltpu.VMEM((LAG, 2, order, 2 * BLOCK), jnp.bfloat16),
            pltpu.VMEM((order, order), jnp.bfloat16),
            pltpu.VMEM((order, order), jnp.bfloat16),
            pltpu.VMEM((order, 128), jnp.float32),
            dma((owners + 7,)),
            dma((owners - 1,)),
            dma((owners - 1,)),
            dma((owners - 1,)),
            dma((owners - 1,)),
            dma((groups - 1,)),
            dma((groups - 1,)),
            dma((owners - 1,)),
            dma((owners - 1,)),
        ],
        compiler_params=pltpu.CompilerParams(
            collective_id=0, has_side_effects=True, vmem_limit_bytes=16 * 1024 * 1024 + 40 * order * order
        ),
        name="soap",
    )(
        *[pltpu.with_memory_space_constraint(v, pltpu.HBM) for v in (table, grad[0], left_stat[0, 0], right_stat[0, 0], left_basis[0, 0], right_basis[0, 0],
        row_moment[0], col_moment[0])]
    )
    update, row_next, col_next = pl.pallas_call(
        store_kernel,
        out_shape=tuple(jax.ShapeDtypeStruct(a.shape, a.dtype) for a in (update, row_next, col_next)),
        in_specs=[vmem] * 3,
        out_specs=[hbm] * 3,
        scratch_shapes=[dma((3,))],
        compiler_params=pltpu.CompilerParams(vmem_limit_bytes=4 * 1024 * 1024),
        name="store",
    )(update, row_next, col_next)
    return (update[None], row_next[None], col_next[None])


def solution(mesh):
    in_specs = (
        P("grp", "fsdp", None),
        P("grp", None),
        P("grp", "fsdp", None, None),
        P("grp", "fsdp", None, None),
        P("grp", "fsdp", None, None),
        P("grp", "fsdp", None, None),
        P("grp", "fsdp", None),
        P("grp", "fsdp", None),
    )
    out_specs = (P("grp", "fsdp", None), P("grp", "fsdp", None), P("grp", "fsdp", None))
    return jax.shard_map(shards, mesh=mesh, in_specs=in_specs, out_specs=out_specs, check_vma=False)
```
